32 devices in a mesh: dp: 2 (over x), tp: 16 (over y, z, core).
Axes of the slice: x: 2, y: 2, z: 4, core: 2. Of those that a mesh axis runs over, the one named last changes fastest.
Arguments:
- x: bfloat16 [4096, 14336], P('dp'), parts along dimension 0
- gain: bfloat16 [14336], replicated
- wq: bfloat16 [14336, 14336], P(None, 'tp')
- wk: bfloat16 [14336, 14336], P(None, 'tp')
- wv: bfloat16 [14336, 14336], P(None, 'tp')
- wo: bfloat16 [14336, 14336], P('tp')
Outputs:
- output: bfloat16 [4096, 14336], P('dp'), parts along dimension 0
There are 2 independent parts. The reference program is written for one: setup_inputs(seed, part) draws one part's arguments, and reference() takes and returns one part's arrays. A program takes and returns all parts, laid end to end along the dimension named above; an argument that names none is the same for every part.
All inputs are finite; a program needn't handle non-finite values.
Results may differ from the reference program's by a relative error of at most 0.012.
Values are sent between devices in bfloat16 or wider.
A program may use at most 2 GiB of HBM per device.

```python
import jax
import jax.numpy as jnp
from jax import lax

ROWS = 2048
D = 14336
HEADS = 112
KV_HEADS = 112
HEAD = 128
THETA = 10000


def setup_inputs(seed: int = 0, part: int = 0) -> dict:
    kx, kn, kq, kk, kv, ko = jax.random.split(jax.random.key(seed), 6)

    def weights(key, rows, columns):
        return jax.random.normal(key, (rows, columns), jnp.float32) * rows**-0.5

    drawn = {
        "x": jax.random.normal(jax.random.fold_in(kx, part), (ROWS, D), jnp.float32),
        "gain": 1 + 0.1 * jax.random.normal(kn, (D,), jnp.float32),
        "wq": 2 * weights(kq, D, HEADS * HEAD),
        "wk": 2 * weights(kk, D, KV_HEADS * HEAD),
        "wv": 4 * weights(kv, D, KV_HEADS * HEAD),
        "wo": weights(ko, HEADS * HEAD, D),
    }
    return {k: v.astype(jnp.bfloat16) for k, v in drawn.items()}


def normed(x, gain):
    wide = x.astype(jnp.float32)
    scale = lax.rsqrt(jnp.mean(wide * wide, -1, keepdims=True) + 1e-6)
    return (wide * scale * gain.astype(jnp.float32)).astype(jnp.bfloat16)


def turned(t, place, theta):
    half = t.shape[-1] // 2
    angle = place.astype(jnp.float32)[:, None] * theta ** (-jnp.arange(half, dtype=jnp.float32) / half)
    cos, sin = jnp.cos(angle)[:, None], jnp.sin(angle)[:, None]
    a, b = t[..., :half].astype(jnp.float32), t[..., half:].astype(jnp.float32)
    return jnp.concatenate([a * cos - b * sin, b * cos + a * sin], -1).astype(jnp.bfloat16)


def matmul(a, w):
    return jnp.dot(a, w, preferred_element_type=jnp.float32).astype(jnp.bfloat16)


def einsum(form, a, b):
    return jnp.einsum(form, a.astype(jnp.float32), b.astype(jnp.float32))


def attention(q, k, v):
    scores = einsum("tgsd,ugd->gstu", q, k) * q.shape[-1] ** -0.5
    token = jnp.arange(q.shape[0])
    scores = jnp.where(token[:, None] >= token, scores, -jnp.inf)
    weights = jax.nn.softmax(scores, -1).astype(jnp.bfloat16)
    return einsum("gstu,ugd->tgsd", weights, v).astype(jnp.bfloat16)


def reference(x, gain, wq, wk, wv, wo):
    a, place = normed(x, gain), jnp.arange(ROWS)
    q = turned(matmul(a, wq).reshape(ROWS, HEADS, HEAD), place, THETA).reshape(ROWS, KV_HEADS, -1, HEAD)
    k = turned(matmul(a, wk).reshape(ROWS, KV_HEADS, HEAD), place, THETA)
    v = matmul(a, wv).reshape(ROWS, KV_HEADS, HEAD)
    seen = attention(q, k, v).reshape(ROWS, HEADS * HEAD)
    return (x.astype(jnp.float32) + jnp.dot(seen, wo, preferred_element_type=jnp.float32)).astype(jnp.bfloat16)
```

```python
import functools, math
import jax, jax.numpy as jnp
from jax import lax
from jax.experimental import pallas as pl
from jax.experimental.pallas import tpu as pltpu
from jax.sharding import PartitionSpec as P
MESH = pl.DeviceIdType.MESH
BF, F32 = jnp.bfloat16, jnp.float32
PER = 10
Z_AT, B_AT, K_AT = (1, 3, 6, 9), (2, 5, 8), {1: 0, 3: 1, 6: 2, 9: 3}
Y_, M_, P_ = 0, 1, 2


def w32(c, a=1, b=0):
    return jnp.where(c, jnp.int32(a), jnp.int32(b))


def tables(y, z):
    t = dict(height=0, deep=0, root=0, cy=0, cm=0, cp=0, out=0, dist=0)
    mid = (z == 1) | (z == 2)
    for p in range(PER):
        if p in Z_AT:
            k = K_AT[p]
            lo, hi = z < k, z > k
            height = jnp.where(lo, z, jnp.where(hi, 3 - z, max(k, 3 - k)))
            root = w32(z == k)
            cy, cm, cp = 0, w32((z > 0) & (z <= k)), w32((z < 3) & (z >= k))
            out = jnp.where(lo, P_, jnp.where(hi, M_, Y_))
            dist = jnp.where(lo, k - z, z - k)
            deep = int(max(k, 3 - k) == 3)
        else:
            s = 1 if p in B_AT else 0
            spine = y == s
            height = jnp.where(spine, w32(mid, 2, 1), 0)
            root = w32(spine & mid)
            cy, cm, cp = w32(spine), w32(spine & (z == 1)), w32(spine & (z == 2))
            out = jnp.where(spine, w32(z < 2, P_, M_), Y_)
            dist = jnp.where(spine, w32(mid, 0, 1), w32(mid, 1, 2))
            deep = 0
        for name, v, bits in (("height", height, 2), ("deep", deep, 1), ("root", root, 1), ("cy", cy, 1), ("cm", cm, 1), ("cp", cp, 1), ("out", out, 2), ("dist", dist, 2)):
            t[name] = t[name] + v * (1 << (bits * p))
    return t


def engine(cfg, refs):
    N, C, RB, NB, NS, AL = cfg["N"], cfg["C"], cfg["RB"], cfg["NB"], cfg["NS"], cfg["AL"]
    BPC = cfg["MC"] // RB
    r = refs
    i = lax.axis_index("tp")
    c, z, y = i % 2, (i // 2) % 4, i // 8
    dev = lambda y, z, c: (y * 4 + z) * 2 + c
    near = [dev(1 - y, z, c), dev(y, jnp.maximum(z - 1, 0), c), dev(y, jnp.minimum(z + 1, 3), c), dev(y, z, 1 - c)]
    T = tables(y, z)
    col = pl.multiple_of(c * C, 128)
    mine = pl.ds(col, C)

    def place(b):
        b = jnp.clip(b, 0, NB - 1)
        return b - 10 * lax.shift_right_logical(b * 205, 11)

    def get(name, p):
        bits = 2 if name in ("height", "out", "dist") else 1
        return lax.shift_right_logical(T[name], p * bits) & ((1 << bits) - 1)

    def rows(b):
        return pl.ds(pl.multiple_of(b * RB, RB), RB)

    def remote(src, dst, ss, rs, to):
        return pltpu.make_async_remote_copy(src, dst, ss, rs, device_id={"tp": to}, device_id_type=MESH)

    def barrier():
        bar = pltpu.get_barrier_semaphore()
        for d in (0, 3):
            pl.semaphore_signal(bar, inc=1, device_id={"tp": near[d]}, device_id_type=MESH)
        for d, ok in ((1, z > 0), (2, z < 3)):
            @pl.when(ok)
            def _():
                pl.semaphore_signal(bar, inc=1, device_id={"tp": near[d]}, device_id_type=MESH)
        pl.semaphore_wait(bar, 2 + w32(z > 0) + w32(z < 3))

    def valid(b):
        return (b >= 0) & (b < NB)

    def got(d, b):
        remote(r["send"].at[0], r["rbuf"].at[d, rows(b)], r["ssem"].at[0], r["rsem"].at[d, b], near[0]).wait_recv()

    def fetch_reduce(b, h):
        p = place(b)

        @pl.when(valid(b) & (get("height", p) == h))
        def _():
            pltpu.make_async_copy(r["d2d"].at[rows(b)], r["vbuf"].at[h, 0], r["vsem"].at[h, 0]).start()
            if h:
                d0 = jnp.where(get("cy", p) == 1, 0, jnp.where(get("cm", p) == 1, 1, 2))
                got(d0, b)
                pltpu.make_async_copy(r["rbuf"].at[d0, rows(b)], r["vbuf"].at[h, 1], r["vsem"].at[h, 1]).start()
            if h >= 2:
                @pl.when(get("cy", p) + get("cm", p) + get("cp", p) == 2)
                def _():
                    d1 = jnp.where(get("cp", p) == 1, 2, 1)
                    got(d1, b)
                    pltpu.make_async_copy(r["rbuf"].at[d1, rows(b)], r["vbuf"].at[h, 2], r["vsem"].at[h, 2]).start()

    def reduce(b, h):
        p = place(b)

        @pl.when(valid(b) & (get("height", p) == h))
        def _():
            slot = lax.rem(b, NS)
            half = lax.shift_right_logical(b, int(math.log2(BPC))) & 1
            local = pl.ds(pl.multiple_of((b & (BPC - 1)) * RB, RB), RB)
            n = get("cy", p) + get("cm", p) + get("cp", p)
            for j in range(2 if h else 1):
                pltpu.make_async_copy(r["d2d"].at[rows(b)], r["vbuf"].at[h, j], r["vsem"].at[h, j]).wait()

            @pl.when(b >= NS)
            def _():
                remote(r["send"].at[slot], r["rbuf"].at[0, rows(b)], r["ssem"].at[slot], r["rsem"].at[0, b], near[0]).wait_send()

            def add(n):
                step = cfg["STEP"]

                def body(i, _):
                    at = pl.ds(pl.multiple_of(i * step, step), step)
                    s = r["part"][half, local, at] + r["vbuf"][h, 0, :, at].astype(F32)
                    for j in range(n):
                        s = s + r["vbuf"][h, 1 + j, :, at].astype(F32)
                    r["send"][slot, :, at] = s.astype(BF)
                lax.fori_loop(0, C // step, body, None)

            if h == 0:
                add(0)
            elif h == 1:
                add(1)
            else:
                @pl.when(n == 1)
                def _():
                    add(1)

                @pl.when(n == 2)
                def _():
                    pltpu.make_async_copy(r["d2d"].at[rows(b)], r["vbuf"].at[h, 2], r["vsem"].at[h, 2]).wait()
                    add(2)
            o = get("out", p)
            opp = jnp.where(o == 0, 0, 3 - o)
            to = jnp.where(o == 0, near[0], jnp.where(o == 1, near[1], near[2]))
            remote(r["send"].at[slot], r["rbuf"].at[opp, rows(b)], r["ssem"].at[slot], r["rsem"].at[opp, b], to).start()

    def fetch_final(b, deep):
        p = place(b)

        @pl.when(valid(b) & (get("root", p) == 1) & (get("deep", p) == deep))
        def _():
            pltpu.make_async_copy(r["x"].at[rows(b), mine], r["xbuf"].at[deep], r["xsem"].at[deep]).start()
            o = get("out", p)
            got(o, b)
            pltpu.make_async_copy(r["rbuf"].at[o, rows(b)], r["ebuf"].at[deep], r["esem"].at[deep]).start()

    def spread(src, b, p, q, local):
        dst = r["out"].at[rows(b), mine]
        for d, name in ((0, "cy"), (1, "cm"), (2, "cp")):
            @pl.when(get(name, p) == 1)
            def _():
                remote(src, dst, r["bsem"].at[d, q], r["zsem"].at[b], near[d]).start()
        remote(src, dst, r["bsem"].at[3, q], r["psem"].at[lax.shift_right_logical(b, int(math.log2(BPC)))], near[3]).start()
        if local:
            pltpu.make_async_copy(src, dst, r["lsem"].at[q]).start()

    def spread_wait(b, p, q, local):
        src = r["fin"].at[q]
        dst = r["out"].at[rows(b), mine]
        for d, name in ((0, "cy"), (1, "cm"), (2, "cp")):
            @pl.when(get(name, p) == 1)
            def _():
                remote(src, dst, r["bsem"].at[d, q], r["zsem"].at[b], near[d]).wait_send()
        remote(src, dst, r["bsem"].at[3, q], r["psem"].at[0], near[3]).wait_send()
        if local:
            pltpu.make_async_copy(src, dst, r["lsem"].at[q]).wait()

    def final(b, deep):
        p = place(b)

        @pl.when(valid(b) & (get("root", p) == 1) & (get("deep", p) == deep))
        def _():
            slot = lax.rem(b, NS)
            pltpu.make_async_copy(r["x"].at[rows(b), mine], r["xbuf"].at[deep], r["xsem"].at[deep]).wait()
            pltpu.make_async_copy(r["rbuf"].at[0, rows(b)], r["ebuf"].at[deep], r["esem"].at[deep]).wait()

            @pl.when(b >= PER)
            def _():
                spread_wait(b - PER, p, p, True)
            step = cfg["STEP"]

            def body(i, _):
                at = pl.ds(pl.multiple_of(i * step, step), step)
                s = r["send"][slot, :, at].astype(F32) + r["ebuf"][deep, :, at].astype(F32)
                r["fin"][p, :, at] = (r["xbuf"][deep, :, at].astype(F32) + s).astype(BF)
            lax.fori_loop(0, C // step, body, None)
            spread(r["fin"].at[p], b, p, p, True)

    def forward(b, lag):
        p = place(b)
        mylag = 3 + get("deep", p) + get("dist", p)

        @pl.when(valid(b) & (get("root", p) == 0) & (mylag == lag))
        def _():
            dst = r["out"].at[rows(b), mine]
            remote(r["fin"].at[0], dst, r["bsem"].at[3, 0], r["zsem"].at[b], near[3]).wait_recv()

            @pl.when(b >= PER)
            def _():
                spread_wait(b - PER, p, p, False)
            spread(dst, b, p, p, False)

    def tick(t):
        for h in range(4):
            reduce(t - 1 - AL * h, h)
        for deep in (0, 1):
            final(t - 1 - AL * (3 + deep), deep)
        for lag in (4, 5, 6, 7):
            forward(t - AL * lag, lag)
        for h in range(4):
            fetch_reduce(t - AL * h, h)
        for deep in (0, 1):
            fetch_final(t - AL * (3 + deep), deep)

    def finish():
        def last(j, _):
            b = NB - PER + j
            p = place(b)

            @pl.when(get("root", p) == 1)
            def _():
                spread_wait(b, p, p, True)

            @pl.when(get("root", p) == 0)
            def _():
                spread_wait(b, p, p, False)
        lax.fori_loop(0, PER, last, None)

        def sent(j, _):
            remote(r["send"].at[j], r["rbuf"].at[0, rows(j)], r["ssem"].at[j], r["rsem"].at[0, j], near[0]).wait_send()
        lax.fori_loop(0, NS, sent, None)
        other = pl.ds(pl.multiple_of((1 - c) * C, 128), C)

        def theirs(j, _):
            at = pl.ds(pl.multiple_of(j * cfg["MC"], cfg["MC"]), cfg["MC"])
            remote(r["out"].at[at, other], r["out"].at[at, other], r["bsem"].at[3, 0], r["psem"].at[j], near[3]).wait_recv()
        lax.fori_loop(0, N // cfg["MC"], theirs, None)

    return dict(tick=tick, finish=finish, barrier=barrier, near=near, c=c, ticks=NB + 7 * AL + 2, remote=remote, mine=mine)


def comm_scratch(cfg):
    C, RB, NB, NS, MC = cfg["C"], cfg["RB"], cfg["NB"], cfg["NS"], cfg["MC"]
    D = pltpu.SemaphoreType.DMA
    return dict(
        send=pltpu.VMEM((NS, RB, C), BF), vbuf=pltpu.VMEM((4, 3, RB, C), BF), ebuf=pltpu.VMEM((2, RB, C), BF), xbuf=pltpu.VMEM((2, RB, C), BF),
        fin=pltpu.VMEM((PER, RB, C), BF), part=pltpu.VMEM((2, MC, C), F32),
        ssem=D((NS,)), rsem=D((3, NB)), vsem=D((4, 3)), esem=D((2,)), xsem=D((2,)), zsem=D((NB,)), bsem=D((4, PER)), lsem=D((PER,)),
        psem=D((cfg["N"] // MC,)), dsem=D((cfg["N"] // MC,)), osem=D((2,)), stsem=D((2,)),
    )


HD = 128
NEG = -1e30
HIDDEN = 2 * NEG
LOG2E = 1.4426950408889634


def dot(a, b, ca=1, cb=0):
    return lax.dot_general(a, b, (((ca,), (cb,)), ((), ())), preferred_element_type=F32)


def config(N, D, nh, KT, QT, NT, AL, NS):
    C = D // 2
    cfg = dict(N=N, D=D, C=C, nh=nh, KT=KT, QT=QT, NT=NT, AL=AL, NS=NS, RB=16, NB=N // 16, MC=256, STEP=512 if C % 512 == 0 else 128)
    cfg["QS"] = D // (KT * QT)
    cfg["NCH"] = N // 256
    cfg["OT"] = C // NT
    cfg["U"] = 1 + cfg["QS"] + cfg["NCH"] + 2 * cfg["OT"]
    cfg["WS"] = 3
    return cfg


def kernel(cfg, names, *refs):
    x, gain, cs, wq, wk, wv, wo, out, rbuf, d2d = refs[:10]
    r = dict(zip(names, refs[10:]))
    r.update(x=x, out=out, rbuf=rbuf, d2d=d2d)
    N, D, C, nh, KT, QT, NT, MC = (cfg[k] for k in ("N", "D", "C", "nh", "KT", "QT", "NT", "MC"))
    QS, NCH, OT, U, AL, WS = (cfg[k] for k in ("QS", "NCH", "OT", "U", "AL", "WS"))
    W = nh * HD
    BPC = MC // cfg["RB"]
    e = engine(cfg, r)
    c, near = e["c"], e["near"]
    A0, P0, O0 = 1 + QS, 1 + QS + NCH, 1 + QS + NCH + OT
    done = lambda u: jnp.minimum(BPC, lax.div(u * (BPC + 1), U))
    assert min(BPC, O0 * (BPC + 1) // U) >= 3 * AL + 1, (O0 * (BPC + 1) // U)
    tiles, wtiles = QS * QT, 2 * OT

    def chunk(w):
        return pl.ds(pl.multiple_of(w * MC, MC), MC)

    def load_x(w):
        return pltpu.make_async_copy(x.at[chunk(w)], r["a"], r["asem"].at[0])

    def load_cs(w):
        return pltpu.make_async_copy(cs.at[chunk(w)], r["cs"], r["asem"].at[1])

    def w_start(s):
        t = lax.rem(s, tiles)
        slot = lax.rem(s, WS)
        at = pl.ds(pl.multiple_of(t * KT, KT), KT)
        for n, ref in enumerate((wq, wk, wv)):
            pltpu.make_async_copy(ref.at[at], r["w"].at[slot, :, pl.ds(n * W, W)], r["wsem"].at[slot]).start()

    def w_wait(s):
        slot = lax.rem(s, WS)
        pltpu.make_async_copy(r["w"].at[slot], r["w"].at[slot], r["wsem"].at[slot]).wait()

    def wo_start(s):
        t = lax.rem(s, wtiles)
        slot = lax.rem(s, WS)
        half = jnp.where(t < OT, 1 - c, c)
        at = pl.multiple_of(half * C + lax.rem(t, OT) * NT, 128)
        pltpu.make_async_copy(wo.at[:, pl.ds(at, NT)], r["wo"].at[slot], r["wosem"].at[slot]).start()

    def wo_wait(s):
        slot = lax.rem(s, WS)
        pltpu.make_async_copy(r["wo"].at[slot], r["wo"].at[slot], r["wosem"].at[slot]).wait()

    def norm(w):
        load_x(w).wait()
        G, S = 16, cfg["STEP"]

        def group(g, _):
            at = pl.ds(pl.multiple_of(g * G, G), G)

            def squares(i, acc):
                v = r["a"][at, pl.ds(pl.multiple_of(i * S, S), S)].astype(F32)
                v = v * v
                for n in range(S // 128):
                    acc = acc + v[:, n * 128:(n + 1) * 128]
                return acc
            acc = lax.fori_loop(0, D // S, squares, jnp.zeros((G, 128), F32))
            scale = lax.rsqrt(jnp.sum(acc, axis=1, keepdims=True) * (1 / D) + 1e-6)

            def apply(i, _):
                cols = pl.ds(pl.multiple_of(i * S, S), S)
                v = r["a"][at, cols].astype(F32)
                r["a"][at, cols] = (v * scale * gain[:, cols].astype(F32)).astype(BF)
            lax.fori_loop(0, D // S, apply, None)
        lax.fori_loop(0, MC // G, group, None)

    def project(w, u):
        def sub(j, _):
            t = (u - 1) * QT + j
            s = w * tiles + t
            w_wait(s)
            part = dot(r["a"][:, pl.ds(pl.multiple_of(t * KT, KT), KT)], r["w"][lax.rem(s, WS)])

            @pl.when(t == 0)
            def _():
                r["acc"][...] = part

            @pl.when(t > 0)
            def _():
                r["acc"][...] += part

            @pl.when(s + WS < tiles * NCH)
            def _():
                w_start(s + WS)
        lax.fori_loop(0, QT, sub, None)

    def turn(w):
        load_cs(w).wait()
        t = r["cs"][...]
        swapped = pltpu.roll(t, 64, 1)
        low = lax.broadcasted_iota(jnp.int32, t.shape, 1) < 64
        cosf, sinf = jnp.where(low, t, swapped), jnp.where(low, -swapped, t)

        def turned(at):
            v = r["acc"][:, at:at + HD].astype(BF).astype(F32)
            return (v * cosf + pltpu.roll(v, 64, 1) * sinf).astype(BF)
        for h in range(nh):
            cols = slice(h * HD, (h + 1) * HD)
            r["q"][:, cols] = turned(h * HD)
            r["k"][chunk(w), cols] = turned(W + h * HD)
            r["vt"][h, :HD, chunk(w)] = r["acc"][:, 2 * W + h * HD:2 * W + (h + 1) * HD].astype(BF).T
        r["top"][...] = jnp.full(r["top"].shape, NEG, F32)
        r["mix"][...] = jnp.zeros(r["mix"].shape, F32)

    def attend(w, j, diagonal):
        scale = HD ** -0.5 * LOG2E
        keys = chunk(j)
        scores = [dot(r["k"][keys, h * HD:(h + 1) * HD], r["q"][:, h * HD:(h + 1) * HD], 1, 1) for h in range(nh)]
        weights, keeps = [], []
        for h, s in enumerate(scores):
            if diagonal:
                ok = lax.broadcasted_iota(jnp.int32, s.shape, 1) >= lax.broadcasted_iota(jnp.int32, s.shape, 0)
                s = jnp.where(ok, s, HIDDEN)
            old = r["top"][h:h + 1, :]
            top = jnp.maximum(old, s.max(axis=0, keepdims=True))
            r["top"][h:h + 1, :] = top
            weights.append(jnp.exp2((s - top) * scale).astype(BF))
            keeps.append(jnp.exp2((old - top) * scale))
        for h, (p, keep) in enumerate(zip(weights, keeps)):
            r["mix"][h] = r["mix"][h] * keep + dot(r["vt"][h, :, keys], p)

    def settle():
        for h in range(nh):
            r["o"][:, h * HD:(h + 1) * HD] = (r["mix"][h, :HD] * (1 / r["mix"][h, HD:HD + 1])).T.astype(BF)

    def send_d2d(w, n, slot):
        cols = pl.ds(pl.multiple_of(n * NT, 128), NT)
        return e["remote"](r["stage"].at[slot], d2d.at[chunk(w), cols], r["stsem"].at[slot], r["dsem"].at[w], near[3])

    def project_out(w, u):
        n = u - P0
        s = w * wtiles + n
        wo_wait(s)
        part = dot(r["o"][...], r["wo"][lax.rem(s, WS)])

        @pl.when(u < O0)
        def _():
            slot = lax.rem(n, 2)

            @pl.when(n >= 2)
            def _():
                send_d2d(w, n, slot).wait_send()
            r["stage"][slot] = part.astype(BF)
            send_d2d(w, n, slot).start()

        @pl.when(u >= O0)
        def _():
            @pl.when(u < O0 + 2)
            def _():
                send_d2d(w, 0, u - O0).wait_send()
            at = pl.ds(pl.multiple_of((n - OT) * NT, 128), NT)
            r["part"][lax.rem(w, 2), :, at] = part

        @pl.when(s + WS < wtiles * NCH)
        def _():
            wo_start(s + WS)

    load_x(0).start()
    load_cs(0).start()
    for s in range(WS):
        w_start(jnp.int32(s))
        wo_start(jnp.int32(s))
    r["vt"][:, HD:, :] = jnp.ones((nh, r["vt"].shape[1] - HD, N), BF)
    e["barrier"]()

    def tick(t):
        @pl.when((lax.rem(t, BPC) == 0) & (t < cfg["NB"]))
        def _():
            j = lax.div(t, BPC)
            half = d2d.at[chunk(j)]
            e["remote"](half, half, r["stsem"].at[0], r["dsem"].at[j], near[3]).wait_recv()
        e["tick"](t)

    steps = U * NCH

    def body(g, _):
        w = lax.div(g, U)
        u = g - w * U
        work = g < steps

        @pl.when(work & (u == 0))
        def _():
            norm(w)

        @pl.when(work & (u >= 1) & (u < A0))
        def _():
            project(w, u)

        @pl.when(work & (u == A0 - 1))
        def _():
            turn(w)

            @pl.when(w + 1 < NCH)
            def _():
                load_x(w + 1).start()
                load_cs(w + 1).start()

        @pl.when(work & (u >= A0) & (u < A0 + w))
        def _():
            attend(w, u - A0, False)

        @pl.when(work & (u == A0 + w))
        def _():
            attend(w, w, True)
            settle()

        @pl.when(work & (u >= P0))
        def _():
            project_out(w, u)

        base = (w - 1) * BPC
        first = jnp.where(work, base + done(u), (NCH - 1) * BPC + g - steps)
        last = jnp.where(work, jnp.where(w > 0, base + done(u + 1), first), first + 1)
        lax.fori_loop(first, last, lambda t, _: tick(t), None)
    total = e["ticks"]
    lax.fori_loop(0, steps + total - (NCH - 1) * BPC, body, None)
    e["finish"]()


def scratch(cfg):
    N, D, C, nh, KT, NT, MC, WS = (cfg[k] for k in ("N", "D", "C", "nh", "KT", "NT", "MC", "WS"))
    W = nh * HD
    D_ = pltpu.SemaphoreType.DMA
    sc = comm_scratch(cfg)
    sc.update(
        a=pltpu.VMEM((MC, D), BF), cs=pltpu.VMEM((MC, HD), F32), acc=pltpu.VMEM((MC, 3 * W), F32), w=pltpu.VMEM((WS, KT, 3 * W), BF),
        wo=pltpu.VMEM((WS, W, NT), BF), q=pltpu.VMEM((MC, W), BF), k=pltpu.VMEM((N, W), BF), vt=pltpu.VMEM((nh, HD + 16, N), BF),
        top=pltpu.VMEM((nh, MC), F32), mix=pltpu.VMEM((nh, HD + 16, MC), F32), o=pltpu.VMEM((MC, W), BF), stage=pltpu.VMEM((2, MC, NT), BF),
        asem=D_((2,)), wsem=D_((WS,)), wosem=D_((WS,)))
    return sc


def layer(cfg):
    N, D, C, nh = cfg["N"], cfg["D"], cfg["C"], cfg["nh"]
    sc = scratch(cfg)
    hbm = pl.BlockSpec(memory_space=pltpu.HBM)

    def f(x, gain, wq, wk, wv, wo):
        half = HD // 2
        angle = jnp.arange(N).astype(F32)[:, None] * 10000 ** (-jnp.arange(half, dtype=F32) / half)
        cs = jnp.concatenate([jnp.cos(angle), jnp.sin(angle)], 1)
        out, _, _ = pl.pallas_call(
            functools.partial(kernel, cfg, list(sc)),
            out_shape=[jax.ShapeDtypeStruct((N, D), BF), jax.ShapeDtypeStruct((3, N, C), BF), jax.ShapeDtypeStruct((N, C), BF)],
            in_specs=[hbm, pl.BlockSpec(memory_space=pltpu.VMEM)] + [hbm] * 5, out_specs=[hbm] * 3,
            scratch_shapes=list(sc.values()),
            compiler_params=pltpu.CompilerParams(collective_id=3, has_side_effects=True, vmem_limit_bytes=67043328), name="layer")(
                x, gain.reshape(1, D), cs, wq, wk, wv, wo)
        return out
    return f


def solution(mesh):
    tp = mesh.shape["tp"]

    def step(x, gain, wq, wk, wv, wo):
        N, D = x.shape
        return layer(config(N, D, wq.shape[1] // HD, KT=512, QT=4, NT=1024, AL=4, NS=20))(x, gain, wq, wk, wv, wo)

    tokens, columns = P("dp", None), P(None, "tp")
    return jax.shard_map(
        step,
        mesh=mesh,
        in_specs=(tokens, P(None), columns, columns, columns, P("tp", None)),
        out_specs=tokens,
        check_vma=False,
    )
```

```python
import functools, math
import numpy as np
import jax, jax.numpy as jnp
from jax import lax
from jax.experimental import pallas as pl
from jax.experimental.pallas import tpu as pltpu
from jax.sharding import PartitionSpec as P
MESH = pl.DeviceIdType.MESH
BF, F32 = jnp.bfloat16, jnp.float32
PER = 10
Z_AT, B_AT, K_AT = (1, 3, 6, 9), (2, 5, 8), {1: 0, 3: 1, 6: 2, 9: 3}
Y_, M_, P_ = 0, 1, 2


def w32(c, a=1, b=0):
    return jnp.where(c, jnp.int32(a), jnp.int32(b))


def tables(y, z):
    t = dict(height=0, deep=0, root=0, cy=0, cm=0, cp=0, out=0, dist=0)
    mid = (z == 1) | (z == 2)
    for p in range(PER):
        if p in Z_AT:
            k = K_AT[p]
            lo, hi = z < k, z > k
            height = jnp.where(lo, z, jnp.where(hi, 3 - z, max(k, 3 - k)))
            root = w32(z == k)
            cy, cm, cp = 0, w32((z > 0) & (z <= k)), w32((z < 3) & (z >= k))
            out = jnp.where(lo, P_, jnp.where(hi, M_, Y_))
            dist = jnp.where(lo, k - z, z - k)
            deep = int(max(k, 3 - k) == 3)
        else:
            s = 1 if p in B_AT else 0
            spine = y == s
            height = jnp.where(spine, w32(mid, 2, 1), 0)
            root = w32(spine & mid)
            cy, cm, cp = w32(spine), w32(spine & (z == 1)), w32(spine & (z == 2))
            out = jnp.where(spine, w32(z < 2, P_, M_), Y_)
            dist = jnp.where(spine, w32(mid, 0, 1), w32(mid, 1, 2))
            deep = 0
        for name, v, bits in (("height", height, 2), ("deep", deep, 1), ("root", root, 1), ("cy", cy, 1), ("cm", cm, 1), ("cp", cp, 1), ("out", out, 2), ("dist", dist, 2)):
            t[name] = t[name] + v * (1 << (bits * p))
    return t


def engine(cfg, refs):
    N, C, RB, NB, NS, AL = cfg["N"], cfg["C"], cfg["RB"], cfg["NB"], cfg["NS"], cfg["AL"]
    BPC = cfg["MC"] // RB
    r = refs
    i = lax.axis_index("tp")
    c, z, y = i % 2, (i // 2) % 4, i // 8
    dev = lambda y, z, c: (y * 4 + z) * 2 + c
    near = [dev(1 - y, z, c), dev(y, jnp.maximum(z - 1, 0), c), dev(y, jnp.minimum(z + 1, 3), c), dev(y, z, 1 - c)]
    T = tables(y, z)
    col = pl.multiple_of(c * C, 128)
    mine = pl.ds(col, C)

    shift = cfg["SHIFT"] * c

    def place(b):
        b = jnp.clip(b, 0, NB - 1) + shift
        return b - 10 * lax.shift_right_logical(b * 205, 11)

    def get(name, p):
        bits = 2 if name in ("height", "out", "dist") else 1
        return lax.shift_right_logical(T[name], p * bits) & ((1 << bits) - 1)

    def rows(b):
        return pl.ds(pl.multiple_of(b * RB, RB), RB)

    def remote(src, dst, ss, rs, to):
        return pltpu.make_async_remote_copy(src, dst, ss, rs, device_id={"tp": to}, device_id_type=MESH)

    def barrier():
        bar = pltpu.get_barrier_semaphore()
        for d in (0, 3):
            pl.semaphore_signal(bar, inc=1, device_id={"tp": near[d]}, device_id_type=MESH)
        for d, ok in ((1, z > 0), (2, z < 3)):
            @pl.when(ok)
            def _():
                pl.semaphore_signal(bar, inc=1, device_id={"tp": near[d]}, device_id_type=MESH)
        pl.semaphore_wait(bar, 2 + w32(z > 0) + w32(z < 3))

    def valid(b):
        return (b >= 0) & (b < NB)

    def got(d, b):
        remote(r["send"].at[0], r["rbuf"].at[d, rows(b)], r["ssem"].at[0], r["rsem"].at[d, b], near[0]).wait_recv()

    def fetch_reduce(b, h):
        p = place(b)

        @pl.when(valid(b) & (get("height", p) == h))
        def _():
            pltpu.make_async_copy(r["d2d"].at[rows(b)], r["vbuf"].at[h, 0], r["vsem"].at[h, 0]).start()
            if h:
                d0 = jnp.where(get("cy", p) == 1, 0, jnp.where(get("cm", p) == 1, 1, 2))
                got(d0, b)
                pltpu.make_async_copy(r["rbuf"].at[d0, rows(b)], r["vbuf"].at[h, 1], r["vsem"].at[h, 1]).start()
            if h >= 2:
                @pl.when(get("cy", p) + get("cm", p) + get("cp", p) == 2)
                def _():
                    d1 = jnp.where(get("cp", p) == 1, 2, 1)
                    got(d1, b)
                    pltpu.make_async_copy(r["rbuf"].at[d1, rows(b)], r["vbuf"].at[h, 2], r["vsem"].at[h, 2]).start()

    def reduce(b, h):
        p = place(b)

        @pl.when(valid(b) & (get("height", p) == h))
        def _():
            slot = lax.rem(b, NS)
            half = lax.shift_right_logical(b, int(math.log2(BPC))) & 1
            local = pl.ds(pl.multiple_of((b & (BPC - 1)) * RB, RB), RB)
            n = get("cy", p) + get("cm", p) + get("cp", p)
            for j in range(2 if h else 1):
                pltpu.make_async_copy(r["d2d"].at[rows(b)], r["vbuf"].at[h, j], r["vsem"].at[h, j]).wait()

            @pl.when(b >= NS)
            def _():
                remote(r["send"].at[slot], r["rbuf"].at[0, rows(b)], r["ssem"].at[slot], r["rsem"].at[0, b], near[0]).wait_send()

            def add(n):
                step = cfg["STEP"]

                def body(i, _):
                    at = pl.ds(pl.multiple_of(i * step, step), step)
                    s = r["part"][half, local, at] + r["vbuf"][h, 0, :, at].astype(F32)
                    for j in range(n):
                        s = s + r["vbuf"][h, 1 + j, :, at].astype(F32)
                    r["send"][slot, :, at] = s.astype(BF)
                lax.fori_loop(0, C // step, body, None)

            if h == 0:
                add(0)
            elif h == 1:
                add(1)
            else:
                @pl.when(n == 1)
                def _():
                    add(1)

                @pl.when(n == 2)
                def _():
                    pltpu.make_async_copy(r["d2d"].at[rows(b)], r["vbuf"].at[h, 2], r["vsem"].at[h, 2]).wait()
                    add(2)
            o = get("out", p)
            opp = jnp.where(o == 0, 0, 3 - o)
            to = jnp.where(o == 0, near[0], jnp.where(o == 1, near[1], near[2]))
            remote(r["send"].at[slot], r["rbuf"].at[opp, rows(b)], r["ssem"].at[slot], r["rsem"].at[opp, b], to).start()

    def fetch_final(b, deep):
        p = place(b)

        @pl.when(valid(b) & (get("root", p) == 1) & (get("deep", p) == deep))
        def _():
            pltpu.make_async_copy(r["x"].at[rows(b), mine], r["xbuf"].at[deep], r["xsem"].at[deep]).start()
            o = get("out", p)
            got(o, b)
            pltpu.make_async_copy(r["rbuf"].at[o, rows(b)], r["ebuf"].at[deep], r["esem"].at[deep]).start()

    def spread(src, b, p, q, local):
        dst = r["out"].at[rows(b), mine]
        for d, name in ((0, "cy"), (1, "cm"), (2, "cp")):
            @pl.when(get(name, p) == 1)
            def _():
                remote(src, dst, r["bsem"].at[d, q], r["zsem"].at[b], near[d]).start()
        remote(src, dst, r["bsem"].at[3, q], r["psem"].at[lax.shift_right_logical(b, int(math.log2(BPC)))], near[3]).start()
        if local:
            pltpu.make_async_copy(src, dst, r["lsem"].at[q]).start()

    def spread_wait(b, p, q, local):
        src = r["fin"].at[q]
        dst = r["out"].at[rows(b), mine]
        for d, name in ((0, "cy"), (1, "cm"), (2, "cp")):
            @pl.when(get(name, p) == 1)
            def _():
                remote(src, dst, r["bsem"].at[d, q], r["zsem"].at[b], near[d]).wait_send()
        remote(src, dst, r["bsem"].at[3, q], r["psem"].at[0], near[3]).wait_send()
        if local:
            pltpu.make_async_copy(src, dst, r["lsem"].at[q]).wait()

    def final(b, deep):
        p = place(b)

        @pl.when(valid(b) & (get("root", p) == 1) & (get("deep", p) == deep))
        def _():
            slot = lax.rem(b, NS)
            pltpu.make_async_copy(r["x"].at[rows(b), mine], r["xbuf"].at[deep], r["xsem"].at[deep]).wait()
            pltpu.make_async_copy(r["rbuf"].at[0, rows(b)], r["ebuf"].at[deep], r["esem"].at[deep]).wait()

            @pl.when(b >= PER)
            def _():
                spread_wait(b - PER, p, p, True)
            step = cfg["STEP"]

            def body(i, _):
                at = pl.ds(pl.multiple_of(i * step, step), step)
                s = r["send"][slot, :, at].astype(F32) + r["ebuf"][deep, :, at].astype(F32)
                r["fin"][p, :, at] = (r["xbuf"][deep, :, at].astype(F32) + s).astype(BF)
            lax.fori_loop(0, C // step, body, None)
            spread(r["fin"].at[p], b, p, p, True)

    def forward(b, lag):
        p = place(b)
        mylag = 3 + get("deep", p) + get("dist", p)

        @pl.when(valid(b) & (get("root", p) == 0) & (mylag == lag))
        def _():
            dst = r["out"].at[rows(b), mine]
            remote(r["fin"].at[0], dst, r["bsem"].at[3, 0], r["zsem"].at[b], near[3]).wait_recv()

            @pl.when(b >= PER)
            def _():
                spread_wait(b - PER, p, p, False)
            spread(dst, b, p, p, False)

    def tick(t):
        for h in range(4):
            reduce(t - 1 - AL * h, h)
        for deep in (0, 1):
            final(t - 1 - AL * (3 + deep), deep)
        for lag in (4, 5, 6, 7):
            forward(t - AL * lag, lag)
        for h in range(4):
            fetch_reduce(t - AL * h, h)
        for deep in (0, 1):
            fetch_final(t - AL * (3 + deep), deep)

    def finish():
        def last(j, _):
            b = NB - PER + j
            p = place(b)

            @pl.when(get("root", p) == 1)
            def _():
                spread_wait(b, p, p, True)

            @pl.when(get("root", p) == 0)
            def _():
                spread_wait(b, p, p, False)
        lax.fori_loop(0, PER, last, None)

        def sent(j, _):
            remote(r["send"].at[j], r["rbuf"].at[0, rows(j)], r["ssem"].at[j], r["rsem"].at[0, j], near[0]).wait_send()
        lax.fori_loop(0, NS, sent, None)
        other = pl.ds(pl.multiple_of((1 - c) * C, 128), C)

        def theirs(j, _):
            at = pl.ds(pl.multiple_of(j * cfg["MC"], cfg["MC"]), cfg["MC"])
            remote(r["out"].at[at, other], r["out"].at[at, other], r["bsem"].at[3, 0], r["psem"].at[j], near[3]).wait_recv()
        lax.fori_loop(0, N // cfg["MC"], theirs, None)

    return dict(tick=tick, finish=finish, barrier=barrier, near=near, c=c, ticks=NB + 7 * AL + 2, remote=remote, mine=mine)


def comm_scratch(cfg):
    C, RB, NB, NS, MC = cfg["C"], cfg["RB"], cfg["NB"], cfg["NS"], cfg["MC"]
    D = pltpu.SemaphoreType.DMA
    return dict(
        send=pltpu.VMEM((NS, RB, C), BF), vbuf=pltpu.VMEM((4, 3, RB, C), BF), ebuf=pltpu.VMEM((2, RB, C), BF), xbuf=pltpu.VMEM((2, RB, C), BF),
        fin=pltpu.VMEM((PER, RB, C), BF), part=pltpu.VMEM((2, MC, C), F32),
        ssem=D((NS,)), rsem=D((3, NB)), vsem=D((4, 3)), esem=D((2,)), xsem=D((2,)), zsem=D((NB,)), bsem=D((4, PER)), lsem=D((PER,)),
        psem=D((cfg["N"] // MC,)), dsem=D((cfg["N"] // MC,)), osem=D((2,)), stsem=D((4,)),
    )


HD = 128
THETA = 10000
NEG = -1e30
HIDDEN = 2 * NEG
LOG2E = 1.4426950408889634


def dot(a, b, ca=1, cb=0):
    return lax.dot_general(a, b, (((ca,), (cb,)), ((), ())), preferred_element_type=F32)


def config(N, D, nh, KT, NT, AL, NS):
    C = D // 2
    cfg = dict(N=N, D=D, C=C, nh=nh, KT=KT, NT=NT, AL=AL, NS=NS, RB=16, NB=N // 16, MC=256, STEP=512 if C % 512 == 0 else 128)
    cfg["QS"] = D // (2 * KT)
    cfg["NCH"] = N // 256
    cfg["OT"] = C // NT
    cfg["U"] = 1 + cfg["QS"] + cfg["NCH"] + cfg["OT"]
    cfg.update(SHIFT=5, WS=5, SD=min(4, cfg["OT"]), NSTEP=2048 if D % 2048 == 0 else 512, TN=2, TQ=17, TA=5, TO=13)
    return cfg


def kernel(cfg, names, *refs):
    x, gain, cs, wq, wk, wv, wo, out, rbuf, d2d = refs[:10]
    r = dict(zip(names, refs[10:]))
    r.update(x=x, out=out, rbuf=rbuf, d2d=d2d)
    N, D, C, nh, KT, NT, MC = (cfg[k] for k in ("N", "D", "C", "nh", "KT", "NT", "MC"))
    QS, NCH, OT, U, AL, WS, SD = (cfg[k] for k in ("QS", "NCH", "OT", "U", "AL", "WS", "SD"))
    W = nh * HD
    K1 = 512 if W > 512 else W // 2
    BPC = MC // cfg["RB"]
    e = engine(cfg, r)
    c, near = e["c"], e["near"]
    A0, P0 = 1 + QS, 1 + QS + NCH
    spans = ((0, cfg["TN"]), (1, cfg["TQ"]), (A0, cfg["TA"]), (P0, cfg["TO"]), (U, 0))
    whole = sum(t * (b[0] - a) for (a, t), b in zip(spans, spans[1:]))

    def done(u):
        at = sum(t * jnp.clip(u - a, 0, b[0] - a) for (a, t), b in zip(spans, spans[1:]))
        return lax.div(at * BPC + whole // 2, whole)
    tiles = 2 * QS + 2 * OT

    tiles = 2 * QS + 2 * OT

    def chunk(w):
        return pl.ds(pl.multiple_of(w * MC, MC), MC)

    def load_x(w):
        return pltpu.make_async_copy(x.at[chunk(w)], r["a"], r["asem"].at[0])

    def load_cs(w):
        return pltpu.make_async_copy(cs.at[chunk(w)], r["cs"], r["asem"].at[1])

    def w_start(s):
        t = lax.rem(s, tiles)
        slot = lax.rem(s, WS)

        @pl.when(t < 2 * QS)
        def _():
            at = pl.ds(pl.multiple_of(t * KT, KT), KT)
            for n, ref in enumerate((wq, wk, wv)):
                pltpu.make_async_copy(ref.at[at], r["w"].at[slot, :, pl.ds(n * W, W)], r["wsem"].at[slot]).start(priority=1)

        @pl.when(t >= 2 * QS)
        def _():
            n = t - 2 * QS
            half = jnp.where(n < OT, 1 - c, c)
            at = pl.ds(pl.multiple_of(half * C + lax.rem(n, OT) * NT, 128), NT)
            for i, (a, b) in enumerate(((0, K1), (K1, W))):
                pltpu.make_async_copy(wo.at[pl.ds(a, b - a), at], r["w"].at[slot, pl.ds(0, b - a), pl.ds(i * NT, NT)], r["wsem"].at[slot]).start(priority=1)

    def w_wait(s, rows, cols):
        slot = lax.rem(s, WS)
        view = r["w"].at[slot, pl.ds(0, rows), pl.ds(0, cols)]
        pltpu.make_async_copy(view, view, r["wsem"].at[slot]).wait()

    def w_more(s):
        @pl.when(s + WS < tiles * NCH)
        def _():
            w_start(s + WS)

    def squares(at, rows, into):
        acc = [jnp.zeros((rows, 128), F32)] * 4
        for n in range(D // 128):
            v = r["a"][at, n * 128:(n + 1) * 128].astype(F32)
            acc[n % 4] = acc[n % 4] + v * v
        r["sums"][into, :] = (acc[0] + acc[1]) + (acc[2] + acc[3])

    def rescale():
        total = jnp.sum(r["sums"][...], axis=1, keepdims=True)
        r["scale"][...] = jnp.broadcast_to(lax.rsqrt(total * (1 / D) + 1e-6), r["scale"].shape)
        r["acc"][...] = jnp.zeros(r["acc"].shape, F32)
        normed(0, "even")

    def normed(t, into):
        cols = pl.ds(pl.multiple_of(t * KT, KT), KT)
        v = r["a"][:, cols].astype(F32) * jnp.concatenate([r["scale"][...]] * (KT // 128), 1)
        r[into][...] = (v.reshape(MC // 8, 8, KT) * r["gain8"][:, cols]).reshape(MC, KT).astype(BF)

    def project(w, u):
        t = 2 * (u - 1)
        s = w * tiles + t
        w_wait(s, KT, 3 * W)
        w_wait(s + 1, KT, 3 * W)
        normed(t + 1, "odd")
        r["acc"][...] += dot(r["even"][...], r["w"][lax.rem(s, WS)])
        normed(jnp.minimum(t + 2, 2 * QS - 1), "even")
        r["acc"][...] += dot(r["odd"][...], r["w"][lax.rem(s + 1, WS)])
        w_more(s)
        w_more(s + 1)

    def turn(w):
        load_cs(w).wait()
        t = r["cs"][...]
        swapped = pltpu.roll(t, 64, 1)
        low = lax.broadcasted_iota(jnp.int32, t.shape, 1) < 64
        cosf, sinf = jnp.where(low, t, swapped), jnp.where(low, -swapped, t)

        def turned(at):
            v = r["acc"][:, at:at + HD].astype(BF).astype(F32)
            return (v * cosf + pltpu.roll(v, 64, 1) * sinf).astype(BF)
        for h in range(nh):
            cols = slice(h * HD, (h + 1) * HD)
            r["q"][:, cols] = turned(h * HD)
            r["k"][chunk(w), cols] = turned(W + h * HD)
            r["vt"][h, :HD, chunk(w)] = r["acc"][:, 2 * W + h * HD:2 * W + (h + 1) * HD].astype(BF).T
        r["top"][...] = jnp.full(r["top"].shape, NEG, F32)
        r["mix"][...] = jnp.zeros(r["mix"].shape, F32)

    def attend(w, j, diagonal):
        scale = HD ** -0.5 * LOG2E
        keys = chunk(j)
        scores = [dot(r["k"][keys, h * HD:(h + 1) * HD], r["q"][:, h * HD:(h + 1) * HD], 1, 1) for h in range(nh)]
        weights, keeps = [], []
        for h, s in enumerate(scores):
            if diagonal:
                ok = lax.broadcasted_iota(jnp.int32, s.shape, 1) >= lax.broadcasted_iota(jnp.int32, s.shape, 0)
                s = jnp.where(ok, s, HIDDEN)
            old = r["top"][h:h + 1, :]
            top = jnp.maximum(old, s.max(axis=0, keepdims=True))
            r["top"][h:h + 1, :] = top
            weights.append(jnp.exp2((s - top) * scale).astype(BF))
            keeps.append(jnp.exp2((old - top) * scale))
        for h, (p, keep) in enumerate(zip(weights, keeps)):
            r["mix"][h] = r["mix"][h] * keep + dot(r["vt"][h, :, keys], p)

    def settle():
        for h in range(nh):
            r["o"][:, h * HD:(h + 1) * HD] = (r["mix"][h, :HD] * (1 / r["mix"][h, HD:HD + 1])).T.astype(BF)

    def send_d2d(w, n, slot):
        cols = pl.ds(pl.multiple_of(n * NT, 128), NT)
        return e["remote"](r["stage"].at[slot], d2d.at[chunk(w), cols], r["stsem"].at[slot], r["dsem"].at[w], near[3])

    def product(s):
        w = r["w"].at[lax.rem(s, WS)]
        return dot(r["o"][:, :K1], w[:K1, :NT]) + dot(r["o"][:, K1:], w[:W - K1, NT:2 * NT])

    def project_out(w, u):
        k = u - P0
        n = 2 * k
        s = w * tiles + 2 * QS + n

        @pl.when((k == 0) & (w + 1 < NCH))
        def _():
            load_x(w + 1).wait()
        w_wait(s, W // 2, 2 * NT)
        w_wait(s + 1, W // 2, 2 * NT)
        share = -(-MC // 16 // OT) * 16
        at = pl.ds(pl.multiple_of(jnp.minimum(k * share, MC - share), 16), share)

        def own(n):
            return pl.ds(pl.multiple_of((n - OT) * NT, 128), NT)

        def tile(m, mine):
            if mine:
                r["part"][lax.rem(w, 2), :, own(m)] = product(s + m - n)
            else:
                r["stage"][lax.rem(m, SD)] = product(s + m - n).astype(BF)

        for m in (n, n + 1):
            @pl.when((m >= SD) & (m < OT + SD))
            def _():
                send_d2d(w, m - SD, lax.rem(m, SD)).wait_send()

        @pl.when(n + 1 < OT)
        def _():
            tile(n, False)
            tile(n + 1, False)
            squares(at, share, at)
            send_d2d(w, n, lax.rem(n, SD)).start()
            send_d2d(w, n + 1, lax.rem(n + 1, SD)).start()

        if OT % 2:
            @pl.when(n + 1 == OT)
            def _():
                tile(n, False)
                tile(n + 1, True)
                squares(at, share, at)
                send_d2d(w, n, lax.rem(n, SD)).start()

        @pl.when(n >= OT)
        def _():
            tile(n, True)
            tile(n + 1, True)
            squares(at, share, at)
        w_more(s)
        w_more(s + 1)

    load_x(0).start()
    load_cs(0).start()
    for s in range(WS):
        w_start(jnp.int32(s))
    for n in range(D // 128):
        r["gain8"][:, n * 128:(n + 1) * 128] = jnp.broadcast_to(gain[n:n + 1, :].astype(F32), (8, 128))
    r["vt"][:, HD:, :] = jnp.ones((nh, r["vt"].shape[1] - HD, N), BF)
    e["barrier"]()
    load_x(0).wait()

    def some(g, _):
        at = pl.ds(pl.multiple_of(g * 16, 16), 16)
        squares(at, 16, at)
    lax.fori_loop(0, MC // 16, some, None)

    def tick(t):
        @pl.when((lax.rem(t, BPC) == 0) & (t < cfg["NB"]))
        def _():
            j = lax.div(t, BPC)
            half = d2d.at[chunk(j)]
            e["remote"](half, half, r["stsem"].at[0], r["dsem"].at[j], near[3]).wait_recv()
        e["tick"](t)

    steps = U * NCH

    def body(g, _):
        w = lax.div(g, U)
        u = g - w * U
        work = g < steps

        @pl.when(work & (u == 0))
        def _():
            rescale()

        @pl.when(work & (u >= 1) & (u < A0))
        def _():
            project(w, u)

        @pl.when(work & (u == A0 - 1))
        def _():
            turn(w)

            @pl.when(w + 1 < NCH)
            def _():
                load_x(w + 1).start(priority=1)
                load_cs(w + 1).start()

        @pl.when(work & (u >= A0) & (u < A0 + w))
        def _():
            attend(w, u - A0, False)

        @pl.when(work & (u == A0 + w))
        def _():
            attend(w, w, True)
            settle()

        @pl.when(work & (u >= P0))
        def _():
            project_out(w, u)

        base = (w - 1) * BPC
        first = jnp.where(work, base + done(u), (NCH - 1) * BPC + g - steps)
        last = jnp.where(work, jnp.where(w > 0, base + done(u + 1), first), first + 1)
        lax.fori_loop(first, last, lambda t, _: tick(t), None)
    total = e["ticks"]
    lax.fori_loop(0, steps + total - (NCH - 1) * BPC, body, None)
    e["finish"]()


def scratch(cfg):
    N, D, C, nh, KT, NT, MC, WS = (cfg[k] for k in ("N", "D", "C", "nh", "KT", "NT", "MC", "WS"))
    W = nh * HD
    D_ = pltpu.SemaphoreType.DMA
    sc = comm_scratch(cfg)
    sc.update(
        a=pltpu.VMEM((MC, D), BF), gain8=pltpu.VMEM((8, D), F32), sums=pltpu.VMEM((MC, 128), F32), scale=pltpu.VMEM((MC, 128), F32),
        even=pltpu.VMEM((MC, KT), BF), odd=pltpu.VMEM((MC, KT), BF), cs=pltpu.VMEM((MC, HD), F32), acc=pltpu.VMEM((MC, 3 * W), F32),
        w=pltpu.VMEM((WS, KT, 3 * W), BF), q=pltpu.VMEM((MC, W), BF), k=pltpu.VMEM((N, W), BF), vt=pltpu.VMEM((nh, HD + 16, N), BF),
        top=pltpu.VMEM((nh, MC), F32), mix=pltpu.VMEM((nh, HD + 16, MC), F32), o=pltpu.VMEM((MC, W), BF), stage=pltpu.VMEM((cfg["SD"], MC, NT), BF),
        asem=D_((2,)), wsem=D_((WS,)))
    return sc


def layer(cfg):
    N, D, C, nh = cfg["N"], cfg["D"], cfg["C"], cfg["nh"]
    sc = scratch(cfg)
    hbm = pl.BlockSpec(memory_space=pltpu.HBM)

    def f(x, gain, wq, wk, wv, wo):
        half = HD // 2
        turn = np.float64(THETA) ** (-np.arange(half) / half)
        angle = (np.arange(N, dtype=np.float32)[:, None] * turn.astype(np.float32)).astype(np.float64)
        cs = jnp.asarray(np.concatenate([np.cos(angle), np.sin(angle)], 1), F32)
        out, _, _ = pl.pallas_call(
            functools.partial(kernel, cfg, list(sc)),
            out_shape=[jax.ShapeDtypeStruct((N, D), BF), jax.ShapeDtypeStruct((3, N, C), BF), jax.ShapeDtypeStruct((N, C), BF)],
            in_specs=[hbm, pl.BlockSpec(memory_space=pltpu.VMEM)] + [hbm] * 5, out_specs=[hbm] * 3,
            scratch_shapes=list(sc.values()),
            compiler_params=pltpu.CompilerParams(collective_id=3, has_side_effects=True, vmem_limit_bytes=67043328), name="layer")(
                x, gain.reshape(D // 128, 128), cs, wq, wk, wv, wo)
        return out
    return f


def solution(mesh):
    tp = mesh.shape["tp"]

    def step(x, gain, wq, wk, wv, wo):
        N, D = x.shape
        return layer(config(N, D, wq.shape[1] // HD, KT=512, NT=1024, AL=4, NS=20))(x, gain, wq, wk, wv, wo)

    tokens, columns = P("dp", None), P(None, "tp")
    return jax.shard_map(
        step,
        mesh=mesh,
        in_specs=(tokens, P(None), columns, columns, columns, P("tp", None)),
        out_specs=tokens,
        check_vma=False,
    )
```

```python
import functools, math
import numpy as np
import jax, jax.numpy as jnp
from jax import lax
from jax.experimental import pallas as pl
from jax.experimental.pallas import tpu as pltpu
from jax.sharding import PartitionSpec as P
MESH = pl.DeviceIdType.MESH
BF, F32 = jnp.bfloat16, jnp.float32
PER = 10
ORDER = ("A", 1, "B", 2, "B", "A", "B", "A", 3, 0)
Z_AT = tuple(p for p in range(PER) if ORDER[p] in (0, 1, 2, 3))
B_AT = tuple(p for p in range(PER) if ORDER[p] == "B")
K_AT = {p: ORDER[p] for p in Z_AT}
Y_, M_, P_ = 0, 1, 2


def w32(c, a=1, b=0):
    return jnp.where(c, jnp.int32(a), jnp.int32(b))


def tables(y, z):
    t = dict(height=0, deep=0, root=0, cy=0, cm=0, cp=0, out=0, dist=0)
    each = []
    mid = (z == 1) | (z == 2)
    for p in range(PER):
        if p in Z_AT:
            k = K_AT[p]
            lo, hi = z < k, z > k
            height = jnp.where(lo, z, jnp.where(hi, 3 - z, max(k, 3 - k)))
            root = w32(z == k)
            cy, cm, cp = 0, w32((z > 0) & (z <= k)), w32((z < 3) & (z >= k))
            out = jnp.where(lo, P_, jnp.where(hi, M_, Y_))
            dist = jnp.where(lo, k - z, z - k)
            deep = int(max(k, 3 - k) == 3)
        else:
            s = 1 if p in B_AT else 0
            spine = y == s
            height = jnp.where(spine, w32(mid, 2, 1), 0)
            root = w32(spine & mid)
            cy, cm, cp = w32(spine), w32(spine & (z == 1)), w32(spine & (z == 2))
            out = jnp.where(spine, w32(z < 2, P_, M_), Y_)
            dist = jnp.where(spine, w32(mid, 0, 1), w32(mid, 1, 2))
            deep = 0
        for name, v, bits in (("height", height, 2), ("deep", deep, 1), ("root", root, 1), ("cy", cy, 1), ("cm", cm, 1), ("cp", cp, 1), ("out", out, 2), ("dist", dist, 2)):
            t[name] = t[name] + v * (1 << (bits * p))
        each.append(dict(height=height, deep=deep, root=root, dist=dist))
    return t, each


def engine(cfg, refs):
    N, C, RB, NB, NS, AL = cfg["N"], cfg["C"], cfg["RB"], cfg["NB"], cfg["NS"], cfg["AL"]
    BPC = cfg["MC"] // RB
    r = refs
    i = lax.axis_index("tp")
    c, z, y = i % 2, (i // 2) % 4, i // 8
    dev = lambda y, z, c: (y * 4 + z) * 2 + c
    near = [dev(1 - y, z, c), dev(y, jnp.maximum(z - 1, 0), c), dev(y, jnp.minimum(z + 1, 3), c), dev(y, z, 1 - c)]
    T, each = tables(y, z)

    def turns(lag, test):
        bits = 0
        for i in range(PER):
            ok = test(each[(i - lag) % PER])
            bits = bits + (int(ok) if isinstance(ok, bool) else w32(ok)) * (1 << i)
        return bits
    reduces = [turns(1 + AL * h, lambda q: q["height"] == h) for h in range(4)]
    finals = [turns(1 + AL * (3 + k), lambda q: (q["root"] == 1) & (q["deep"] == k)) for k in (0, 1)]
    forwards = [turns(AL * lag + cfg["BL"], lambda q: (q["root"] == 0) & (3 + q["deep"] + q["dist"] == lag)) for lag in (4, 5, 6, 7)]
    reduce_fetches = [turns(AL * h, lambda q: q["height"] == h) for h in range(4)]
    final_fetches = [turns(AL * (3 + k), lambda q: (q["root"] == 1) & (q["deep"] == k)) for k in (0, 1)]
    col = pl.multiple_of(c * C, 128)
    mine = pl.ds(col, C)

    shift = cfg["SHIFT"] * c

    def place(b):
        b = jnp.clip(b, 0, NB - 1) + shift
        return b - 10 * lax.shift_right_logical(b * 205, 11)

    def get(name, p):
        bits = 2 if name in ("height", "out", "dist") else 1
        return lax.shift_right_logical(T[name], p * bits) & ((1 << bits) - 1)

    def lap(b):
        return lax.rem(b, min(NB, 64))

    def rows(b):
        return pl.ds(pl.multiple_of(b * RB, RB), RB)

    def remote(src, dst, ss, rs, to):
        return pltpu.make_async_remote_copy(src, dst, ss, rs, device_id={"tp": to}, device_id_type=MESH)

    def barrier():
        bar = pltpu.get_barrier_semaphore()
        for d in (0, 3):
            pl.semaphore_signal(bar, inc=1, device_id={"tp": near[d]}, device_id_type=MESH)
        for d, ok in ((1, z > 0), (2, z < 3)):
            @pl.when(ok)
            def _():
                pl.semaphore_signal(bar, inc=1, device_id={"tp": near[d]}, device_id_type=MESH)

    def met():
        pl.semaphore_wait(pltpu.get_barrier_semaphore(), 2 + w32(z > 0) + w32(z < 3))

    def valid(b):
        return (b >= 0) & (b < NB)

    def got(d, b):
        remote(r["send"].at[0], r["rbuf"].at[d, rows(b)], r["ssem"].at[0], r["rsem"].at[d, lap(b)], near[0]).wait_recv()

    def fetch_reduce(ok, b, h):
        @pl.when(ok & valid(b))
        def _():
            p = place(b)
            pltpu.make_async_copy(r["d2d"].at[rows(b)], r["vbuf"].at[h, 0], r["vsem"].at[h, 0]).start()
            if h:
                d0 = jnp.where(get("cy", p) == 1, 0, jnp.where(get("cm", p) == 1, 1, 2))
                got(d0, b)
                pltpu.make_async_copy(r["rbuf"].at[d0, rows(b)], r["vbuf"].at[h, 1], r["vsem"].at[h, 1]).start()
            if h >= 2:
                @pl.when(get("cy", p) + get("cm", p) + get("cp", p) == 2)
                def _():
                    d1 = jnp.where(get("cp", p) == 1, 2, 1)
                    got(d1, b)
                    pltpu.make_async_copy(r["rbuf"].at[d1, rows(b)], r["vbuf"].at[h, 2], r["vsem"].at[h, 2]).start()

    def reduce(ok, b, h):
        @pl.when(ok & valid(b))
        def _():
            p = place(b)
            slot = lax.rem(b, NS)
            half = lax.shift_right_logical(b, int(math.log2(BPC))) & 1
            local = pl.ds(pl.multiple_of((b & (BPC - 1)) * RB, RB), RB)
            n = get("cy", p) + get("cm", p) + get("cp", p)
            for j in range(2 if h else 1):
                pltpu.make_async_copy(r["d2d"].at[rows(b)], r["vbuf"].at[h, j], r["vsem"].at[h, j]).wait()

            @pl.when(b >= NS)
            def _():
                remote(r["send"].at[slot], r["rbuf"].at[0, rows(b)], r["ssem"].at[slot], r["rsem"].at[0, lap(b)], near[0]).wait_send()

            def add(n):
                step = cfg["STEP"]

                def body(i, _):
                    at = pl.ds(pl.multiple_of(i * step, step), step)
                    s = r["part"][half, local, at] + r["vbuf"][h, 0, :, at].astype(F32)
                    for j in range(n):
                        s = s + r["vbuf"][h, 1 + j, :, at].astype(F32)
                    r["send"][slot, :, at] = s.astype(BF)
                lax.fori_loop(0, C // step, body, None)

            if h == 0:
                add(0)
            elif h == 1:
                add(1)
            else:
                @pl.when(n == 1)
                def _():
                    add(1)

                @pl.when(n == 2)
                def _():
                    pltpu.make_async_copy(r["d2d"].at[rows(b)], r["vbuf"].at[h, 2], r["vsem"].at[h, 2]).wait()
                    add(2)
            o = get("out", p)
            opp = jnp.where(o == 0, 0, 3 - o)
            to = jnp.where(o == 0, near[0], jnp.where(o == 1, near[1], near[2]))
            remote(r["send"].at[slot], r["rbuf"].at[opp, rows(b)], r["ssem"].at[slot], r["rsem"].at[opp, lap(b)], to).start()

    def fetch_final(ok, b, deep):
        @pl.when(ok & valid(b))
        def _():
            p = place(b)
            pltpu.make_async_copy(r["x"].at[rows(b), mine], r["xbuf"].at[deep], r["xsem"].at[deep]).start()
            o = get("out", p)
            got(o, b)
            pltpu.make_async_copy(r["rbuf"].at[o, rows(b)], r["ebuf"].at[deep], r["esem"].at[deep]).start()

    def spread(src, b, p, q, local):
        dst = r["out"].at[rows(b), mine]
        for d, name in ((0, "cy"), (1, "cm"), (2, "cp")):
            @pl.when(get(name, p) == 1)
            def _():
                remote(src, dst, r["bsem"].at[d, q], r["zsem"].at[lap(b)], near[d]).start()
        remote(src, dst, r["bsem"].at[3, q], r["psem"].at[lax.shift_right_logical(b, int(math.log2(BPC)))], near[3]).start()
        if local:
            pltpu.make_async_copy(src, dst, r["lsem"].at[q]).start()

    def spread_wait(b, p, q, local):
        src = r["fin"].at[q]
        dst = r["out"].at[rows(b), mine]
        for d, name in ((0, "cy"), (1, "cm"), (2, "cp")):
            @pl.when(get(name, p) == 1)
            def _():
                remote(src, dst, r["bsem"].at[d, q], r["zsem"].at[lap(b)], near[d]).wait_send()
        remote(src, dst, r["bsem"].at[3, q], r["psem"].at[0], near[3]).wait_send()
        if local:
            pltpu.make_async_copy(src, dst, r["lsem"].at[q]).wait()

    def final(ok, b, deep):
        @pl.when(ok & valid(b))
        def _():
            p = place(b)
            slot = lax.rem(b, NS)
            pltpu.make_async_copy(r["x"].at[rows(b), mine], r["xbuf"].at[deep], r["xsem"].at[deep]).wait()
            pltpu.make_async_copy(r["rbuf"].at[0, rows(b)], r["ebuf"].at[deep], r["esem"].at[deep]).wait()

            @pl.when(b >= PER)
            def _():
                spread_wait(b - PER, p, p, True)
            step = cfg["STEP"]

            def body(i, _):
                at = pl.ds(pl.multiple_of(i * step, step), step)
                s = r["send"][slot, :, at].astype(F32) + r["ebuf"][deep, :, at].astype(F32)
                r["fin"][p, :, at] = (r["xbuf"][deep, :, at].astype(F32) + s).astype(BF)
            lax.fori_loop(0, C // step, body, None)
            spread(r["fin"].at[p], b, p, p, True)

    def forward(ok, b):
        @pl.when(ok & valid(b))
        def _():
            p = place(b)
            dst = r["out"].at[rows(b), mine]
            remote(r["fin"].at[0], dst, r["bsem"].at[3, 0], r["zsem"].at[lap(b)], near[3]).wait_recv()

            @pl.when(b >= PER)
            def _():
                spread_wait(b - PER, p, p, False)
            spread(dst, b, p, p, False)

    def tick(t):
        i = t + shift
        i = i - PER * lax.shift_right_logical(i * 205, 11)

        def on(bits):
            return lax.shift_right_logical(jnp.int32(bits), i) & 1 == 1
        for h in range(4):
            reduce(on(reduces[h]), t - 1 - AL * h, h)
        for k in (0, 1):
            final(on(finals[k]), t - 1 - AL * (3 + k), k)
        for n, lag in enumerate((4, 5, 6, 7)):
            forward(on(forwards[n]), t - AL * lag - cfg["BL"])
        for h in range(4):
            fetch_reduce(on(reduce_fetches[h]), t - AL * h, h)
        for k in (0, 1):
            fetch_final(on(final_fetches[k]), t - AL * (3 + k), k)

    def finish():
        def last(j, _):
            b = NB - PER + j
            p = place(b)

            @pl.when(get("root", p) == 1)
            def _():
                spread_wait(b, p, p, True)

            @pl.when(get("root", p) == 0)
            def _():
                spread_wait(b, p, p, False)
        lax.fori_loop(0, PER, last, None)

        def sent(j, _):
            remote(r["send"].at[j], r["rbuf"].at[0, rows(j)], r["ssem"].at[j], r["rsem"].at[0, lap(j)], near[0]).wait_send()
        lax.fori_loop(0, NS, sent, None)
        other = pl.ds(pl.multiple_of((1 - c) * C, 128), C)

        def theirs(j, _):
            at = pl.ds(pl.multiple_of(j * cfg["MC"], cfg["MC"]), cfg["MC"])
            remote(r["out"].at[at, other], r["out"].at[at, other], r["bsem"].at[3, 0], r["psem"].at[j], near[3]).wait_recv()
        lax.fori_loop(0, N // cfg["MC"], theirs, None)

    return dict(tick=tick, finish=finish, barrier=barrier, met=met, near=near, c=c, ticks=NB + 7 * AL + 2 + cfg["BL"], remote=remote, mine=mine)


def comm_scratch(cfg):
    C, RB, NB, NS, MC = cfg["C"], cfg["RB"], cfg["NB"], cfg["NS"], cfg["MC"]
    D = pltpu.SemaphoreType.DMA
    return dict(
        send=pltpu.VMEM((NS, RB, C), BF), vbuf=pltpu.VMEM((4, 3, RB, C), BF), ebuf=pltpu.VMEM((2, RB, C), BF), xbuf=pltpu.VMEM((2, RB, C), BF),
        fin=pltpu.VMEM((PER, RB, C), BF), part=pltpu.VMEM((2, MC, C), F32),
        ssem=D((NS,)), rsem=D((3, min(NB, 64))), vsem=D((4, 3)), esem=D((2,)), xsem=D((2,)), zsem=D((min(NB, 64),)), bsem=D((4, PER)), lsem=D((PER,)),
        psem=D((cfg["N"] // MC,)), dsem=D((cfg["N"] // MC,)), osem=D((2,)), stsem=D((4,)),
    )


HD = 128
THETA = 10000
NEG = -1e30
HIDDEN = 2 * NEG
LOG2E = 1.4426950408889634


def dot(a, b, ca=1, cb=0):
    return lax.dot_general(a, b, (((ca,), (cb,)), ((), ())), preferred_element_type=F32)


def config(N, D, nh, KT, NT, AL, NS, RB=16):
    C = D // 2
    cfg = dict(N=N, D=D, C=C, nh=nh, KT=KT, NT=NT, AL=AL, NS=NS, RB=RB, NB=N // RB, MC=256, STEP=512 if C % 512 == 0 else 128)
    cfg["QS"] = D // (2 * KT)
    cfg["NCH"] = N // 256
    cfg["OT"] = C // NT
    cfg["U"] = 1 + cfg["QS"] + cfg["NCH"] + cfg["OT"]
    cfg.update(SHIFT=6, BL=2, WS=5, SD=min(4, cfg["OT"]), NSTEP=2048 if D % 2048 == 0 else 512, TN=2, TQ=17, TA=5, TO=12)
    return cfg


def kernel(cfg, names, *refs):
    x, gain, cs, wq, wk, wv, wo, out, rbuf, d2d = refs[:10]
    r = dict(zip(names, refs[10:]))
    r.update(x=x, out=out, rbuf=rbuf, d2d=d2d)
    N, D, C, nh, KT, NT, MC = (cfg[k] for k in ("N", "D", "C", "nh", "KT", "NT", "MC"))
    QS, NCH, OT, U, AL, WS, SD = (cfg[k] for k in ("QS", "NCH", "OT", "U", "AL", "WS", "SD"))
    W = nh * HD
    HT = min(NT, 512)
    K1 = 512 if W > 512 else W // 2
    BPC = MC // cfg["RB"]
    e = engine(cfg, r)
    c, near = e["c"], e["near"]
    A0, P0 = 1 + QS, 1 + QS + NCH
    spans = ((0, cfg["TN"]), (1, cfg["TQ"]), (A0, cfg["TA"]), (P0, cfg["TO"]), (U, 0))
    whole = sum(t * (b[0] - a) for (a, t), b in zip(spans, spans[1:]))

    def done(u):
        at = sum(t * jnp.clip(u - a, 0, b[0] - a) for (a, t), b in zip(spans, spans[1:]))
        return lax.div(at * BPC + whole - 1, whole)
    tiles = 2 * QS + 2 * OT

    tiles = 2 * QS + 2 * OT

    def chunk(w):
        return pl.ds(pl.multiple_of(w * MC, MC), MC)

    def load_x(w):
        return pltpu.make_async_copy(x.at[chunk(w)], r["a"], r["asem"].at[0])

    def load_cs(w):
        return pltpu.make_async_copy(cs.at[chunk(w)], r["cs"], r["asem"].at[1])

    def w_start(s):
        t = lax.rem(s, tiles)
        slot = lax.rem(s, WS)

        @pl.when(t < 2 * QS)
        def _():
            at = pl.ds(pl.multiple_of(t * KT, KT), KT)
            for n, ref in enumerate((wq, wk, wv)):
                pltpu.make_async_copy(ref.at[at], r["w"].at[slot, :, pl.ds(n * W, W)], r["wsem"].at[slot]).start(priority=1)

        @pl.when(t >= 2 * QS)
        def _():
            n = t - 2 * QS
            half = jnp.where(n < OT, 1 - c, c)
            at = pl.ds(pl.multiple_of(half * C + lax.rem(n, OT) * NT, 128), NT)
            for i, (a, b) in enumerate(((0, K1), (K1, W))):
                pltpu.make_async_copy(wo.at[pl.ds(a, b - a), at], r["w"].at[slot, pl.ds(0, b - a), pl.ds(i * NT, NT)], r["wsem"].at[slot]).start(priority=1)

    def w_wait(s, rows, cols):
        slot = lax.rem(s, WS)
        view = r["w"].at[slot, pl.ds(0, rows), pl.ds(0, cols)]
        pltpu.make_async_copy(view, view, r["wsem"].at[slot]).wait()

    def w_more(s):
        @pl.when(s + WS < tiles * NCH)
        def _():
            w_start(s + WS)

    def squares(at, rows, parts):
        acc = [jnp.zeros((rows, 128), F32)] * 4
        for n in range(D // 128):
            v = r["a"][at, n * 128:(n + 1) * 128].astype(F32)
            acc[n % 4] = acc[n % 4] + v * v
            if (n + 1) * parts // (D // 128) > n * parts // (D // 128):
                if n == D // 128 - 1:
                    r["sums"][at, :] = (acc[0] + acc[1]) + (acc[2] + acc[3])
                yield

    def rescale():
        total = jnp.sum(r["sums"][...], axis=1, keepdims=True)
        r["scale"][...] = jnp.broadcast_to(lax.rsqrt(total * (1 / D) + 1e-6), r["scale"].shape)
        r["acc"][...] = jnp.zeros(r["acc"].shape, F32)
        normed(0, "even")

    def normed(t, into):
        cols = pl.ds(pl.multiple_of(t * KT, KT), KT)
        v = r["a"][:, cols].astype(F32) * jnp.concatenate([r["scale"][...]] * (KT // 128), 1)
        r[into][...] = (v.reshape(MC // 8, 8, KT) * r["gain8"][:, cols]).reshape(MC, KT).astype(BF)

    def project(w, u):
        t = 2 * (u - 1)
        s = w * tiles + t
        w_wait(s, KT, 3 * W)
        w_wait(s + 1, KT, 3 * W)
        normed(t + 1, "odd")
        r["acc"][...] += dot(r["even"][...], r["w"][lax.rem(s, WS)])
        normed(jnp.minimum(t + 2, 2 * QS - 1), "even")
        r["acc"][...] += dot(r["odd"][...], r["w"][lax.rem(s + 1, WS)])
        w_more(s)
        w_more(s + 1)

    def turn(w):
        load_cs(w).wait()
        t = r["cs"][...]
        swapped = pltpu.roll(t, 64, 1)
        low = lax.broadcasted_iota(jnp.int32, t.shape, 1) < 64
        cosf, sinf = jnp.where(low, t, swapped), jnp.where(low, -swapped, t)

        def turned(at):
            v = r["acc"][:, at:at + HD].astype(BF).astype(F32)
            return (v * cosf + pltpu.roll(v, 64, 1) * sinf).astype(BF)
        for h in range(nh):
            cols = slice(h * HD, (h + 1) * HD)
            r["q"][:, cols] = turned(h * HD)
            r["k"][chunk(w), cols] = turned(W + h * HD)
            r["vt"][h, :HD, chunk(w)] = r["acc"][:, 2 * W + h * HD:2 * W + (h + 1) * HD].astype(BF).T
        r["top"][...] = jnp.full(r["top"].shape, NEG, F32)
        r["mix"][...] = jnp.zeros(r["mix"].shape, F32)

    def attend(w, j, diagonal):
        scale = HD ** -0.5 * LOG2E
        keys = chunk(j)
        scores = [dot(r["k"][keys, h * HD:(h + 1) * HD], r["q"][:, h * HD:(h + 1) * HD], 1, 1) for h in range(nh)]
        weights, keeps = [], []
        for h, s in enumerate(scores):
            if diagonal:
                ok = lax.broadcasted_iota(jnp.int32, s.shape, 1) >= lax.broadcasted_iota(jnp.int32, s.shape, 0)
                s = jnp.where(ok, s, HIDDEN)
            old = r["top"][h:h + 1, :]
            top = jnp.maximum(old, s.max(axis=0, keepdims=True))
            r["top"][h:h + 1, :] = top
            weights.append(jnp.exp2((s - top) * scale).astype(BF))
            keeps.append(jnp.exp2((old - top) * scale))
        for h, (p, keep) in enumerate(zip(weights, keeps)):
            r["mix"][h] = r["mix"][h] * keep + dot(r["vt"][h, :, keys], p)

    def settle():
        for h in range(nh):
            r["o"][:, h * HD:(h + 1) * HD] = (r["mix"][h, :HD] * (1 / r["mix"][h, HD:HD + 1])).T.astype(BF)

    def send_d2d(w, n, slot):
        cols = pl.ds(pl.multiple_of(n * NT, 128), NT)
        return e["remote"](r["stage"].at[slot], d2d.at[chunk(w), cols], r["stsem"].at[slot], r["dsem"].at[w], near[3])

    def product(s, at):
        w = r["w"].at[lax.rem(s, WS)]
        return dot(r["o"][:, :K1], w[:K1, at:at + HT]) + dot(r["o"][:, K1:], w[:W - K1, NT + at:NT + at + HT])

    def project_out(w, u):
        k = u - P0
        n = 2 * k
        s = w * tiles + 2 * QS + n

        @pl.when((k == 1) & (w + 1 < NCH))
        def _():
            load_x(w + 1).wait()
        w_wait(s, W // 2, 2 * NT)
        w_wait(s + 1, W // 2, 2 * NT)
        share = -(-MC // 16 // (OT - 1)) * 16
        at = pl.ds(pl.multiple_of(jnp.clip((k - 1) * share, 0, MC - share), 16), share)

        def tile(m, mine, beside):
            for i in range(0, NT, HT):
                next(beside, None)
                if mine:
                    r["part"][lax.rem(w, 2), :, pl.ds(pl.multiple_of((m - OT) * NT + i, 128), HT)] = product(s + m - n, i)
                else:
                    r["stage"][lax.rem(m, SD), :, i:i + HT] = product(s + m - n, i).astype(BF)

        def tiles_of(first, second, also=True):
            beside = squares(at, share, 2 * NT // HT) if also else iter(())
            tile(n, first, beside)
            tile(n + 1, second, beside)

        for m in (n, n + 1):
            @pl.when((m >= SD) & (m < OT + SD))
            def _():
                send_d2d(w, m - SD, lax.rem(m, SD)).wait_send()

        @pl.when(k == 0)
        def _():
            tiles_of(False, False, False)

        @pl.when((k > 0) & (n + 1 < OT))
        def _():
            tiles_of(False, False)

        if OT % 2:
            @pl.when(n + 1 == OT)
            def _():
                tiles_of(False, True)

        @pl.when(n >= OT)
        def _():
            tiles_of(True, True)

        for m in (n, n + 1):
            @pl.when(m < OT)
            def _():
                send_d2d(w, m, lax.rem(m, SD)).start()
        w_more(s)
        w_more(s + 1)

    XP = 4
    piece = MC // XP

    def load_piece(g):
        at = pl.ds(pl.multiple_of(g * piece, piece), piece)
        return pltpu.make_async_copy(x.at[at], r["a"].at[at], r["fsem"].at[g])
    for g in range(XP):
        load_piece(g).start()
    e["barrier"]()
    for s in range(2):
        w_start(jnp.int32(s))
    load_cs(0).start()
    for n in range(D // 128):
        r["gain8"][:, n * 128:(n + 1) * 128] = jnp.broadcast_to(gain[n:n + 1, :].astype(F32), (8, 128))
    r["vt"][:, HD:, :] = jnp.ones((nh, r["vt"].shape[1] - HD, N), BF)

    def all_squares(a, b):
        def some(i, _):
            for _ in squares(pl.ds(pl.multiple_of(i * 16, 16), 16), 16, 1):
                pass
        lax.fori_loop(a, b, some, None)

    def first(g, _):
        load_piece(g).wait()
        all_squares(g * (piece // 16), (g + 1) * (piece // 16))
    lax.fori_loop(0, XP, first, None)
    for s in range(2, WS):
        w_start(jnp.int32(s))
    e["met"]()

    def tick(t):
        @pl.when((lax.rem(t, BPC) == 0) & (t < cfg["NB"]))
        def _():
            j = lax.div(t, BPC)
            half = d2d.at[chunk(j)]
            e["remote"](half, half, r["stsem"].at[0], r["dsem"].at[j], near[3]).wait_recv()
        e["tick"](t)

    steps = U * NCH

    def body(g, _):
        w = lax.div(g, U)
        u = g - w * U
        work = g < steps

        base = (w - 1) * BPC
        first = jnp.where(work, base + done(u), (NCH - 1) * BPC + g - steps)
        last = jnp.where(work, jnp.where(w > 0, base + done(u + 1), first), first + 1)
        lax.fori_loop(first, last, lambda t, _: tick(t), None)

        @pl.when(work & (u == 0))
        def _():
            rescale()

        @pl.when(work & (u >= 1) & (u < A0))
        def _():
            project(w, u)

        @pl.when(work & (u == A0 - 1))
        def _():
            turn(w)

            @pl.when(w + 1 < NCH)
            def _():
                load_x(w + 1).start(priority=1)
                load_cs(w + 1).start()

        @pl.when(work & (u >= A0) & (u < A0 + w))
        def _():
            attend(w, u - A0, False)

        @pl.when(work & (u == A0 + w))
        def _():
            attend(w, w, True)
            settle()

        @pl.when(work & (u >= P0))
        def _():
            project_out(w, u)

    total = e["ticks"]
    lax.fori_loop(0, steps + total - (NCH - 1) * BPC, body, None)
    e["finish"]()


def scratch(cfg):
    N, D, C, nh, KT, NT, MC, WS = (cfg[k] for k in ("N", "D", "C", "nh", "KT", "NT", "MC", "WS"))
    W = nh * HD
    D_ = pltpu.SemaphoreType.DMA
    sc = comm_scratch(cfg)
    sc.update(
        a=pltpu.VMEM((MC, D), BF), gain8=pltpu.VMEM((8, D), F32), sums=pltpu.VMEM((MC, 128), F32), scale=pltpu.VMEM((MC, 128), F32),
        even=pltpu.VMEM((MC, KT), BF), odd=pltpu.VMEM((MC, KT), BF), cs=pltpu.VMEM((MC, HD), F32), acc=pltpu.VMEM((MC, 3 * W), F32),
        w=pltpu.VMEM((WS, KT, 3 * W), BF), q=pltpu.VMEM((MC, W), BF), k=pltpu.VMEM((N, W), BF), vt=pltpu.VMEM((nh, HD + 16, N), BF),
        top=pltpu.VMEM((nh, MC), F32), mix=pltpu.VMEM((nh, HD + 16, MC), F32), o=pltpu.VMEM((MC, W), BF), stage=pltpu.VMEM((cfg["SD"], MC, NT), BF),
        asem=D_((2,)), wsem=D_((WS,)), fsem=D_((4,)))
    return sc


def layer(cfg):
    N, D, C, nh = cfg["N"], cfg["D"], cfg["C"], cfg["nh"]
    sc = scratch(cfg)
    hbm = pl.BlockSpec(memory_space=pltpu.HBM)

    def f(x, gain, wq, wk, wv, wo):
        half = HD // 2
        turn = np.float64(THETA) ** (-np.arange(half) / half)
        angle = (np.arange(N, dtype=np.float32)[:, None] * turn.astype(np.float32)).astype(np.float64)
        cs = jnp.asarray(np.concatenate([np.cos(angle), np.sin(angle)], 1), F32)
        out, _, _ = pl.pallas_call(
            functools.partial(kernel, cfg, list(sc)),
            out_shape=[jax.ShapeDtypeStruct((N, D), BF), jax.ShapeDtypeStruct((3, N, C), BF), jax.ShapeDtypeStruct((N, C), BF)],
            in_specs=[hbm, pl.BlockSpec(memory_space=pltpu.VMEM)] + [hbm] * 5, out_specs=[hbm] * 3,
            scratch_shapes=list(sc.values()),
            compiler_params=pltpu.CompilerParams(collective_id=3, has_side_effects=True, vmem_limit_bytes=67043328), name="layer")(
                x, gain.reshape(D // 128, 128), cs, wq, wk, wv, wo)
        return out
    return f


def solution(mesh):
    tp = mesh.shape["tp"]

    def step(x, gain, wq, wk, wv, wo):
        N, D = x.shape
        return layer(config(N, D, wq.shape[1] // HD, KT=512, NT=1024, AL=4, NS=20))(x, gain, wq, wk, wv, wo)

    tokens, columns = P("dp", None), P(None, "tp")
    return jax.shard_map(
        step,
        mesh=mesh,
        in_specs=(tokens, P(None), columns, columns, columns, P("tp", None)),
        out_specs=tokens,
        check_vma=False,
    )
```

```python
import functools, math
import numpy as np
import jax, jax.numpy as jnp
from jax import lax
from jax.experimental import pallas as pl
from jax.experimental.pallas import tpu as pltpu
from jax.sharding import PartitionSpec as P
MESH = pl.DeviceIdType.MESH
BF, F32 = jnp.bfloat16, jnp.float32
PER = 10
ORDER = ("A", 1, "B", 2, "B", "A", "B", "A", 3, 0)
LATE = ("B", 2, "A", "A", 0, "B", "B", "A", "B", 3)
KINDS = ORDER + LATE
Y_, M_, P_ = 0, 1, 2


def w32(c, a=1, b=0):
    return jnp.where(c, jnp.int32(a), jnp.int32(b))


def mask(tests):
    bits = jnp.int32(0)
    for n, ok in enumerate(tests):
        bits = bits + (int(ok) if isinstance(ok, bool) else w32(ok)) * (1 << n)
    return bits


def tables(y, z):
    each = []
    mid = (z == 1) | (z == 2)
    for kind in KINDS:
        if kind in ("A", "B"):
            spine = y == "AB".index(kind)
            each.append(dict(
                height=jnp.where(spine, w32(mid, 2, 1), 0), deep=0, root=spine & mid, cy=spine, cm=spine & (z == 1), cp=spine & (z == 2),
                out=jnp.where(spine, w32(z < 2, P_, M_), Y_), dist=jnp.where(spine, w32(mid, 0, 1), w32(mid, 1, 2))))
        else:
            k = kind
            lo, hi = z < k, z > k
            each.append(dict(
                height=jnp.where(lo, z, jnp.where(hi, 3 - z, max(k, 3 - k))), deep=int(max(k, 3 - k) == 3), root=z == k, cy=False,
                cm=(z > 0) & (z <= k), cp=(z < 3) & (z >= k), out=jnp.where(lo, P_, jnp.where(hi, M_, Y_)), dist=jnp.where(lo, k - z, z - k)))
    return each


def engine(cfg, refs):
    N, C, RB, NB, NS, AL = cfg["N"], cfg["C"], cfg["RB"], cfg["NB"], cfg["NS"], cfg["AL"]
    BPC = cfg["MC"] // RB
    r = refs
    i = lax.axis_index("tp")
    c, z, y = i % 2, (i // 2) % 4, i // 8
    dev = lambda y, z, c: (y * 4 + z) * 2 + c
    near = [dev(1 - y, z, c), dev(y, jnp.maximum(z - 1, 0), c), dev(y, jnp.minimum(z + 1, 3), c), dev(y, z, 1 - c)]
    each = tables(y, z)
    has = {name: mask([q[name] for q in each]) for name in ("cy", "cm", "cp", "root")}
    has.update(out0=mask([q["out"] == M_ for q in each]), out1=mask([q["out"] == P_ for q in each]))
    late = NB - cfg["LATE"]

    def turns(lag, test):
        return mask([test(each[first + (n - lag) % PER]) for first in (0, PER) for n in range(PER)])
    reduces = [turns(1 + AL * h, lambda q: q["height"] == h) for h in range(4)]
    finals = [turns(1 + AL * (3 + k), lambda q: q["root"] & (q["deep"] == k)) for k in (0, 1)]
    forwards = [turns(AL * lag + cfg["BL"], lambda q: ~q["root"] & (3 + q["deep"] + q["dist"] == lag)) for lag in (4, 5, 6, 7)]
    reduce_fetches = [turns(AL * h, lambda q: q["height"] == h) for h in range(4)]
    final_fetches = [turns(AL * (3 + k), lambda q: q["root"] & (q["deep"] == k)) for k in (0, 1)]
    col = pl.multiple_of(c * C, 128)
    mine = pl.ds(col, C)

    shift = cfg["SHIFT"] * c

    def spot(b):
        b = jnp.clip(b, 0, NB - 1) + shift
        return b - PER * lax.shift_right_logical(b * 205, 11)

    def twenty(b):
        return b - 2 * PER * lax.shift_right_logical(b * 205, 12)

    def place(b):
        return spot(b) + jnp.where(b >= late, PER, 0)

    def get(name, p):
        if name == "out":
            return get("out0", p) + 2 * get("out1", p)
        return lax.shift_right_logical(has[name], p) & 1

    def lap(b):
        return lax.rem(b, min(NB, 48))

    def rows(b):
        return pl.ds(pl.multiple_of(b * RB, RB), RB)

    def remote(src, dst, ss, rs, to):
        return pltpu.make_async_remote_copy(src, dst, ss, rs, device_id={"tp": to}, device_id_type=MESH)

    def barrier():
        bar = pltpu.get_barrier_semaphore()
        for d in (0, 3):
            pl.semaphore_signal(bar, inc=1, device_id={"tp": near[d]}, device_id_type=MESH)
        for d, ok in ((1, z > 0), (2, z < 3)):
            @pl.when(ok)
            def _():
                pl.semaphore_signal(bar, inc=1, device_id={"tp": near[d]}, device_id_type=MESH)

    def met():
        pl.semaphore_wait(pltpu.get_barrier_semaphore(), 2 + w32(z > 0) + w32(z < 3))

    def valid(b):
        return (b >= 0) & (b < NB)

    def got(d, b):
        remote(r["send"].at[0], r["rbuf"].at[d, rows(b)], r["ssem"].at[0], r["rsem"].at[d, lap(b)], near[0]).wait_recv()

    def fetch_reduce(ok, b, h):
        @pl.when(ok & valid(b))
        def _():
            p = place(b)
            pltpu.make_async_copy(r["d2d"].at[rows(b)], r["vbuf"].at[h, 0], r["vsem"].at[h, 0]).start()
            if h:
                d0 = jnp.where(get("cy", p) == 1, 0, jnp.where(get("cm", p) == 1, 1, 2))
                got(d0, b)
                pltpu.make_async_copy(r["rbuf"].at[d0, rows(b)], r["vbuf"].at[h, 1], r["vsem"].at[h, 1]).start()
            if h >= 2:
                @pl.when(get("cy", p) + get("cm", p) + get("cp", p) == 2)
                def _():
                    d1 = jnp.where(get("cp", p) == 1, 2, 1)
                    got(d1, b)
                    pltpu.make_async_copy(r["rbuf"].at[d1, rows(b)], r["vbuf"].at[h, 2], r["vsem"].at[h, 2]).start()

    def reduce(ok, b, h):
        @pl.when(ok & valid(b))
        def _():
            p = place(b)
            slot = lax.rem(b, NS)
            half = lax.shift_right_logical(b, int(math.log2(BPC))) & 1
            local = pl.ds(pl.multiple_of((b & (BPC - 1)) * RB, RB), RB)
            n = get("cy", p) + get("cm", p) + get("cp", p)
            for j in range(2 if h else 1):
                pltpu.make_async_copy(r["d2d"].at[rows(b)], r["vbuf"].at[h, j], r["vsem"].at[h, j]).wait()

            @pl.when(b >= NS)
            def _():
                remote(r["send"].at[slot], r["rbuf"].at[0, rows(b)], r["ssem"].at[slot], r["rsem"].at[0, lap(b)], near[0]).wait_send()

            def add(n):
                step = cfg["STEP"]

                def body(i, _):
                    at = pl.ds(pl.multiple_of(i * step, step), step)
                    s = r["part"][half, local, at] + r["vbuf"][h, 0, :, at].astype(F32)
                    for j in range(n):
                        s = s + r["vbuf"][h, 1 + j, :, at].astype(F32)
                    r["send"][slot, :, at] = s.astype(BF)
                lax.fori_loop(0, C // step, body, None)

            if h == 0:
                add(0)
            elif h == 1:
                add(1)
            else:
                @pl.when(n == 1)
                def _():
                    add(1)

                @pl.when(n == 2)
                def _():
                    pltpu.make_async_copy(r["d2d"].at[rows(b)], r["vbuf"].at[h, 2], r["vsem"].at[h, 2]).wait()
                    add(2)
            o = get("out", p)
            opp = jnp.where(o == 0, 0, 3 - o)
            to = jnp.where(o == 0, near[0], jnp.where(o == 1, near[1], near[2]))
            remote(r["send"].at[slot], r["rbuf"].at[opp, rows(b)], r["ssem"].at[slot], r["rsem"].at[opp, lap(b)], to).start()

    def fetch_final(ok, b, deep):
        @pl.when(ok & valid(b))
        def _():
            p = place(b)
            pltpu.make_async_copy(r["x"].at[rows(b), mine], r["xbuf"].at[deep], r["xsem"].at[deep]).start()
            o = get("out", p)
            got(o, b)
            pltpu.make_async_copy(r["rbuf"].at[o, rows(b)], r["ebuf"].at[deep], r["esem"].at[deep]).start()

    def spread(src, b, p, local):
        dst = r["out"].at[rows(b), mine]
        sems, q = (r["bsem"], spot(b)) if local else (r["hsem"], twenty(b))
        for d, name in ((0, "cy"), (1, "cm"), (2, "cp")):
            @pl.when(get(name, p) == 1)
            def _():
                remote(src, dst, sems.at[d, q], r["zsem"].at[lap(b)], near[d]).start()
        remote(src, dst, sems.at[3, q], r["psem"].at[lax.shift_right_logical(b, int(math.log2(BPC)))], near[3]).start()
        if local:
            pltpu.make_async_copy(src, dst, r["lsem"].at[q]).start()

    def spread_wait(b, local):
        p = place(b)
        src, dst = r["fin"].at[spot(b)], r["out"].at[rows(b), mine]
        sems, q = (r["bsem"], spot(b)) if local else (r["hsem"], twenty(b))
        for d, name in ((0, "cy"), (1, "cm"), (2, "cp")):
            @pl.when(get(name, p) == 1)
            def _():
                remote(src, dst, sems.at[d, q], r["zsem"].at[lap(b)], near[d]).wait_send()
        remote(src, dst, sems.at[3, q], r["psem"].at[0], near[3]).wait_send()
        if local:
            pltpu.make_async_copy(src, dst, r["lsem"].at[q]).wait()

    def earlier(b):
        @pl.when((b >= PER) & (get("root", place(b - PER)) == 1))
        def _():
            spread_wait(b - PER, True)

        @pl.when((b >= 2 * PER) & (get("root", place(b - 2 * PER)) == 0))
        def _():
            spread_wait(b - 2 * PER, False)

    def final(ok, b, deep):
        @pl.when(ok & valid(b))
        def _():
            p, q = place(b), spot(b)
            slot = lax.rem(b, NS)
            pltpu.make_async_copy(r["x"].at[rows(b), mine], r["xbuf"].at[deep], r["xsem"].at[deep]).wait()
            pltpu.make_async_copy(r["rbuf"].at[0, rows(b)], r["ebuf"].at[deep], r["esem"].at[deep]).wait()

            earlier(b)
            step = cfg["STEP"]

            def body(i, _):
                at = pl.ds(pl.multiple_of(i * step, step), step)
                s = r["send"][slot, :, at].astype(F32) + r["ebuf"][deep, :, at].astype(F32)
                r["fin"][q, :, at] = (r["xbuf"][deep, :, at].astype(F32) + s).astype(BF)
            lax.fori_loop(0, C // step, body, None)
            spread(r["fin"].at[q], b, p, True)

    def forward(ok, b):
        @pl.when(ok & valid(b))
        def _():
            p = place(b)
            dst = r["out"].at[rows(b), mine]
            remote(r["fin"].at[0], dst, r["hsem"].at[3, 0], r["zsem"].at[lap(b)], near[3]).wait_recv()

            earlier(b)
            spread(dst, b, p, False)

    def tick(t):
        i = t + shift
        i = i - PER * lax.shift_right_logical(i * 205, 11)

        def on(bits, b):
            return lax.shift_right_logical(bits, i + jnp.where(b >= late, PER, 0)) & 1 == 1
        for h in range(4):
            b = t - 1 - AL * h
            reduce(on(reduces[h], b), b, h)
        for k in (0, 1):
            b = t - 1 - AL * (3 + k)
            final(on(finals[k], b), b, k)
        for n, lag in enumerate((4, 5, 6, 7)):
            b = t - AL * lag - cfg["BL"]
            forward(on(forwards[n], b), b)
        for h in range(4):
            b = t - AL * h
            fetch_reduce(on(reduce_fetches[h], b), b, h)
        for k in (0, 1):
            b = t - AL * (3 + k)
            fetch_final(on(final_fetches[k], b), b, k)

    def finish():
        def last(b, _):
            root = get("root", place(b)) == 1

            @pl.when(root & (b >= NB - PER))
            def _():
                spread_wait(b, True)

            @pl.when(~root)
            def _():
                spread_wait(b, False)
        lax.fori_loop(NB - 2 * PER, NB, last, None)

        def sent(j, _):
            remote(r["send"].at[j], r["rbuf"].at[0, rows(j)], r["ssem"].at[j], r["rsem"].at[0, lap(j)], near[0]).wait_send()
        lax.fori_loop(0, NS, sent, None)
        other = pl.ds(pl.multiple_of((1 - c) * C, 128), C)

        def theirs(j, _):
            at = pl.ds(pl.multiple_of(j * cfg["MC"], cfg["MC"]), cfg["MC"])
            remote(r["out"].at[at, other], r["out"].at[at, other], r["bsem"].at[3, 0], r["psem"].at[j], near[3]).wait_recv()
        lax.fori_loop(0, N // cfg["MC"], theirs, None)

    return dict(tick=tick, finish=finish, barrier=barrier, met=met, near=near, c=c, ticks=NB + 7 * AL + 2 + cfg["BL"], remote=remote, mine=mine)


def comm_scratch(cfg):
    C, RB, NB, NS, MC = cfg["C"], cfg["RB"], cfg["NB"], cfg["NS"], cfg["MC"]
    D = pltpu.SemaphoreType.DMA
    return dict(
        send=pltpu.VMEM((NS, RB, C), BF), vbuf=pltpu.VMEM((4, 3, RB, C), BF), ebuf=pltpu.VMEM((2, RB, C), BF), xbuf=pltpu.VMEM((2, RB, C), BF),
        fin=pltpu.VMEM((PER, RB, C), BF), part=pltpu.VMEM((2, MC, C), F32),
        ssem=D((NS,)), rsem=D((3, min(NB, 48))), vsem=D((4, 3)), esem=D((2,)), xsem=D((2,)), zsem=D((min(NB, 48),)), bsem=D((4, PER)), hsem=D((4, 2 * PER)), lsem=D((PER,)),
        psem=D((cfg["N"] // MC,)), dsem=D((cfg["N"] // MC,)), osem=D((2,)), stsem=D((4,)),
    )


HD = 128
THETA = 10000
NEG = -1e30
HIDDEN = 2 * NEG
LOG2E = 1.4426950408889634


def dot(a, b, ca=1, cb=0):
    return lax.dot_general(a, b, (((ca,), (cb,)), ((), ())), preferred_element_type=F32)


def config(N, D, nh, KT, NT, AL, NS, RB=16):
    C = D // 2
    cfg = dict(N=N, D=D, C=C, nh=nh, KT=KT, NT=NT, AL=AL, NS=NS, RB=RB, NB=N // RB, MC=256, STEP=512 if C % 512 == 0 else 128)
    cfg["QS"] = D // (2 * KT)
    cfg["NCH"] = N // 256
    cfg["OT"] = C // NT
    cfg["U"] = 1 + cfg["QS"] + cfg["NCH"] + cfg["OT"]
    cfg.update(SHIFT=6, BL=2, LATE=16, WS=5, SD=min(4, cfg["OT"]), NSTEP=2048 if D % 2048 == 0 else 512, TN=2, TQ=17, TA=5, TO=12)
    return cfg


def kernel(cfg, names, *refs):
    x, gain, cs, wq, wk, wv, wo, out, rbuf, d2d = refs[:10]
    r = dict(zip(names, refs[10:]))
    r.update(x=x, out=out, rbuf=rbuf, d2d=d2d)
    N, D, C, nh, KT, NT, MC = (cfg[k] for k in ("N", "D", "C", "nh", "KT", "NT", "MC"))
    QS, NCH, OT, U, AL, WS, SD = (cfg[k] for k in ("QS", "NCH", "OT", "U", "AL", "WS", "SD"))
    W = nh * HD
    HT = min(NT, 512)
    K1 = 512 if W > 512 else W // 2
    BPC = MC // cfg["RB"]
    e = engine(cfg, r)
    c, near = e["c"], e["near"]
    A0, P0 = 1 + QS, 1 + QS + NCH
    spans = ((0, cfg["TN"]), (1, cfg["TQ"]), (A0, cfg["TA"]), (P0, cfg["TO"]), (U, 0))
    most = sum(t * (b[0] - a) for (a, t), b in zip(spans, spans[1:])) - cfg["TO"]

    def done(u):
        at = sum(t * jnp.clip(u - a, 0, b[0] - a) for (a, t), b in zip(spans, spans[1:]))
        return jnp.where(u == U, BPC + 1, 1 + lax.div(jnp.minimum(at, most) * (BPC - 1) + most - 1, most))
    tiles = 2 * QS + 2 * OT

    tiles = 2 * QS + 2 * OT

    def chunk(w):
        return pl.ds(pl.multiple_of(w * MC, MC), MC)

    def load_x(w):
        return pltpu.make_async_copy(x.at[chunk(w)], r["a"], r["asem"].at[0])

    def load_cs(w):
        return pltpu.make_async_copy(cs.at[chunk(w)], r["cs"], r["asem"].at[1])

    def w_start(s):
        t = lax.rem(s, tiles)
        slot = lax.rem(s, WS)

        @pl.when(t < 2 * QS)
        def _():
            at = pl.ds(pl.multiple_of(t * KT, KT), KT)
            for n, ref in enumerate((wq, wk, wv)):
                pltpu.make_async_copy(ref.at[at], r["w"].at[slot, :, pl.ds(n * W, W)], r["wsem"].at[slot]).start(priority=1)

        @pl.when(t >= 2 * QS)
        def _():
            n = t - 2 * QS
            half = jnp.where(n < OT, 1 - c, c)
            at = pl.ds(pl.multiple_of(half * C + lax.rem(n, OT) * NT, 128), NT)
            for i, (a, b) in enumerate(((0, K1), (K1, W))):
                pltpu.make_async_copy(wo.at[pl.ds(a, b - a), at], r["w"].at[slot, pl.ds(0, b - a), pl.ds(i * NT, NT)], r["wsem"].at[slot]).start(priority=1)

    def w_wait(s, rows, cols):
        slot = lax.rem(s, WS)
        view = r["w"].at[slot, pl.ds(0, rows), pl.ds(0, cols)]
        pltpu.make_async_copy(view, view, r["wsem"].at[slot]).wait()

    def w_more(s):
        @pl.when(s + WS < tiles * NCH)
        def _():
            w_start(s + WS)

    def squares(at, rows, parts):
        acc = [jnp.zeros((rows, 128), F32)] * 4
        for n in range(D // 128):
            v = r["a"][at, n * 128:(n + 1) * 128].astype(F32)
            acc[n % 4] = acc[n % 4] + v * v
            if (n + 1) * parts // (D // 128) > n * parts // (D // 128):
                if n == D // 128 - 1:
                    r["sums"][at, :] = (acc[0] + acc[1]) + (acc[2] + acc[3])
                yield

    def rescale():
        total = jnp.sum(r["sums"][...], axis=1, keepdims=True)
        r["scale"][...] = jnp.broadcast_to(lax.rsqrt(total * (1 / D) + 1e-6), r["scale"].shape)
        r["acc"][...] = jnp.zeros(r["acc"].shape, F32)
        normed(0, "even")

    def normed(t, into):
        cols = pl.ds(pl.multiple_of(t * KT, KT), KT)
        v = r["a"][:, cols].astype(F32) * jnp.concatenate([r["scale"][...]] * (KT // 128), 1)
        r[into][...] = (v.reshape(MC // 8, 8, KT) * r["gain8"][:, cols]).reshape(MC, KT).astype(BF)

    def project(w, u):
        t = 2 * (u - 1)
        s = w * tiles + t
        w_wait(s, KT, 3 * W)
        w_wait(s + 1, KT, 3 * W)
        normed(t + 1, "odd")
        r["acc"][...] += dot(r["even"][...], r["w"][lax.rem(s, WS)])
        normed(jnp.minimum(t + 2, 2 * QS - 1), "even")
        r["acc"][...] += dot(r["odd"][...], r["w"][lax.rem(s + 1, WS)])
        w_more(s)
        w_more(s + 1)

    def turn(w):
        load_cs(w).wait()
        t = r["cs"][...]
        swapped = pltpu.roll(t, 64, 1)
        low = lax.broadcasted_iota(jnp.int32, t.shape, 1) < 64
        cosf, sinf = jnp.where(low, t, swapped), jnp.where(low, -swapped, t)

        def turned(at):
            v = r["acc"][:, at:at + HD].astype(BF).astype(F32)
            return (v * cosf + pltpu.roll(v, 64, 1) * sinf).astype(BF)
        for h in range(nh):
            cols = slice(h * HD, (h + 1) * HD)
            r["q"][:, cols] = turned(h * HD)
            r["k"][chunk(w), cols] = turned(W + h * HD)
            r["vt"][h, :HD, chunk(w)] = r["acc"][:, 2 * W + h * HD:2 * W + (h + 1) * HD].astype(BF).T
        r["top"][...] = jnp.full(r["top"].shape, NEG, F32)
        r["mix"][...] = jnp.zeros(r["mix"].shape, F32)

    def attend(w, j, diagonal):
        scale = HD ** -0.5 * LOG2E
        keys = chunk(j)
        scores = [dot(r["k"][keys, h * HD:(h + 1) * HD], r["q"][:, h * HD:(h + 1) * HD], 1, 1) for h in range(nh)]
        weights, keeps = [], []
        for h, s in enumerate(scores):
            if diagonal:
                ok = lax.broadcasted_iota(jnp.int32, s.shape, 1) >= lax.broadcasted_iota(jnp.int32, s.shape, 0)
                s = jnp.where(ok, s, HIDDEN)
            old = r["top"][h:h + 1, :]
            top = jnp.maximum(old, s.max(axis=0, keepdims=True))
            r["top"][h:h + 1, :] = top
            weights.append(jnp.exp2((s - top) * scale).astype(BF))
            keeps.append(jnp.exp2((old - top) * scale))
        for h, (p, keep) in enumerate(zip(weights, keeps)):
            r["mix"][h] = r["mix"][h] * keep + dot(r["vt"][h, :, keys], p)

    def settle():
        for h in range(nh):
            r["o"][:, h * HD:(h + 1) * HD] = (r["mix"][h, :HD] * (1 / r["mix"][h, HD:HD + 1])).T.astype(BF)

    def send_d2d(w, n, slot):
        cols = pl.ds(pl.multiple_of(n * NT, 128), NT)
        return e["remote"](r["stage"].at[slot], d2d.at[chunk(w), cols], r["stsem"].at[slot], r["dsem"].at[w], near[3])

    def product(s, at):
        w = r["w"].at[lax.rem(s, WS)]
        return dot(r["o"][:, :K1], w[:K1, at:at + HT]) + dot(r["o"][:, K1:], w[:W - K1, NT + at:NT + at + HT])

    def project_out(w, u):
        k = u - P0
        n = 2 * k
        s = w * tiles + 2 * QS + n

        @pl.when((k == 1) & (w + 1 < NCH))
        def _():
            load_x(w + 1).wait()
        w_wait(s, W // 2, 2 * NT)
        w_wait(s + 1, W // 2, 2 * NT)
        share = -(-MC // 16 // (OT - 1)) * 16
        at = pl.ds(pl.multiple_of(jnp.clip((k - 1) * share, 0, MC - share), 16), share)

        def tile(m, mine, beside):
            for i in range(0, NT, HT):
                next(beside, None)
                if mine:
                    r["part"][lax.rem(w, 2), :, pl.ds(pl.multiple_of((m - OT) * NT + i, 128), HT)] = product(s + m - n, i)
                else:
                    r["stage"][lax.rem(m, SD), :, i:i + HT] = product(s + m - n, i).astype(BF)

        def tiles_of(first, second, also=True):
            beside = squares(at, share, 2 * NT // HT) if also else iter(())
            tile(n, first, beside)
            tile(n + 1, second, beside)

        for m in (n, n + 1):
            @pl.when((m >= SD) & (m < OT + SD))
            def _():
                send_d2d(w, m - SD, lax.rem(m, SD)).wait_send()

        @pl.when(k == 0)
        def _():
            tiles_of(False, False, False)

        @pl.when((k > 0) & (n + 1 < OT))
        def _():
            tiles_of(False, False)

        if OT % 2:
            @pl.when(n + 1 == OT)
            def _():
                tiles_of(False, True)

        @pl.when(n >= OT)
        def _():
            tiles_of(True, True)

        for m in (n, n + 1):
            @pl.when(m < OT)
            def _():
                send_d2d(w, m, lax.rem(m, SD)).start()
        w_more(s)
        w_more(s + 1)

    XP = 4
    piece = MC // XP

    def load_piece(g):
        at = pl.ds(pl.multiple_of(g * piece, piece), piece)
        return pltpu.make_async_copy(x.at[at], r["a"].at[at], r["fsem"].at[g])
    for g in range(XP):
        load_piece(g).start()
    e["barrier"]()
    for s in range(2):
        w_start(jnp.int32(s))
    load_cs(0).start()
    for n in range(D // 128):
        r["gain8"][:, n * 128:(n + 1) * 128] = jnp.broadcast_to(gain[n:n + 1, :].astype(F32), (8, 128))
    r["vt"][:, HD:, :] = jnp.ones((nh, r["vt"].shape[1] - HD, N), BF)

    def all_squares(a, b):
        def some(i, _):
            for _ in squares(pl.ds(pl.multiple_of(i * 16, 16), 16), 16, 1):
                pass
        lax.fori_loop(a, b, some, None)

    def first(g, _):
        load_piece(g).wait()
        all_squares(g * (piece // 16), (g + 1) * (piece // 16))
    lax.fori_loop(0, XP, first, None)
    for s in range(2, WS):
        w_start(jnp.int32(s))
    e["met"]()

    def tick(t):
        @pl.when((lax.rem(t, BPC) == 0) & (t < cfg["NB"]))
        def _():
            j = lax.div(t, BPC)
            half = d2d.at[chunk(j)]
            e["remote"](half, half, r["stsem"].at[0], r["dsem"].at[j], near[3]).wait_recv()
        e["tick"](t)

    steps = U * NCH

    def body(g, _):
        w = lax.div(g, U)
        u = g - w * U
        work = g < steps

        base = (w - 1) * BPC
        after = (NCH - 1) * BPC + 1 + g - steps
        first = jnp.where(work, jnp.maximum(base + done(u), 0), after)
        last = jnp.where(work, jnp.maximum(base + done(u + 1), 0), after + 1)
        lax.fori_loop(first, last, lambda t, _: tick(t), None)

        @pl.when(work & (u == 0))
        def _():
            rescale()

        @pl.when(work & (u >= 1) & (u < A0))
        def _():
            project(w, u)

        @pl.when(work & (u == A0 - 1))
        def _():
            turn(w)

            @pl.when(w + 1 < NCH)
            def _():
                load_x(w + 1).start(priority=1)
                load_cs(w + 1).start()

        @pl.when(work & (u >= A0) & (u < A0 + w))
        def _():
            attend(w, u - A0, False)

        @pl.when(work & (u == A0 + w))
        def _():
            attend(w, w, True)
            settle()

        @pl.when(work & (u >= P0))
        def _():
            project_out(w, u)

    total = e["ticks"]
    lax.fori_loop(0, steps + total - (NCH - 1) * BPC - 1, body, None)
    e["finish"]()


def scratch(cfg):
    N, D, C, nh, KT, NT, MC, WS = (cfg[k] for k in ("N", "D", "C", "nh", "KT", "NT", "MC", "WS"))
    W = nh * HD
    D_ = pltpu.SemaphoreType.DMA
    sc = comm_scratch(cfg)
    sc.update(
        a=pltpu.VMEM((MC, D), BF), gain8=pltpu.VMEM((8, D), F32), sums=pltpu.VMEM((MC, 128), F32), scale=pltpu.VMEM((MC, 128), F32),
        even=pltpu.VMEM((MC, KT), BF), odd=pltpu.VMEM((MC, KT), BF), cs=pltpu.VMEM((MC, HD), F32), acc=pltpu.VMEM((MC, 3 * W), F32),
        w=pltpu.VMEM((WS, KT, 3 * W), BF), q=pltpu.VMEM((MC, W), BF), k=pltpu.VMEM((N, W), BF), vt=pltpu.VMEM((nh, HD + 16, N), BF),
        top=pltpu.VMEM((nh, MC), F32), mix=pltpu.VMEM((nh, HD + 16, MC), F32), o=pltpu.VMEM((MC, W), BF), stage=pltpu.VMEM((cfg["SD"], MC, NT), BF),
        asem=D_((2,)), wsem=D_((WS,)), fsem=D_((4,)))
    return sc


def layer(cfg):
    N, D, C, nh = cfg["N"], cfg["D"], cfg["C"], cfg["nh"]
    sc = scratch(cfg)
    hbm = pl.BlockSpec(memory_space=pltpu.HBM)

    def f(x, gain, wq, wk, wv, wo):
        half = HD // 2
        turn = np.float64(THETA) ** (-np.arange(half) / half)
        angle = (np.arange(N, dtype=np.float32)[:, None] * turn.astype(np.float32)).astype(np.float64)
        cs = jnp.asarray(np.concatenate([np.cos(angle), np.sin(angle)], 1), F32)
        out, _, _ = pl.pallas_call(
            functools.partial(kernel, cfg, list(sc)),
            out_shape=[jax.ShapeDtypeStruct((N, D), BF), jax.ShapeDtypeStruct((3, N, C), BF), jax.ShapeDtypeStruct((N, C), BF)],
            in_specs=[hbm, pl.BlockSpec(memory_space=pltpu.VMEM)] + [hbm] * 5, out_specs=[hbm] * 3,
            scratch_shapes=list(sc.values()),
            compiler_params=pltpu.CompilerParams(collective_id=3, has_side_effects=True, vmem_limit_bytes=67043328), name="layer")(
                x, gain.reshape(D // 128, 128), cs, wq, wk, wv, wo)
        return out
    return f


def solution(mesh):
    tp = mesh.shape["tp"]

    def step(x, gain, wq, wk, wv, wo):
        N, D = x.shape
        return layer(config(N, D, wq.shape[1] // HD, KT=512, NT=1024, AL=4, NS=20))(x, gain, wq, wk, wv, wo)

    tokens, columns = P("dp", None), P(None, "tp")
    return jax.shard_map(
        step,
        mesh=mesh,
        in_specs=(tokens, P(None), columns, columns, columns, P("tp", None)),
        out_specs=tokens,
        check_vma=False,
    )
```
